32 devices in a mesh: row: 4 (over x, core), col: 8 (over z, y).
Axes of the slice: x: 2, y: 2, z: 4, core: 2. Of those that a mesh axis runs over, the one named last changes fastest.
Arguments:
- tokens_in: bfloat16 [8192, 2048], P('row', 'col'), may hold values from -6 to 6
- grad_out: bfloat16 [8192, 2048], P('row', 'col'), may hold values from -6 to 6
- sequence_lengths: int32 [4, 32], P('row'), may hold values from 0 to 2048, as said below
- step_count: int32 [1], replicated, may hold values from 2 to 20
- query_key_value: float32 [2048, 6144], P('row', 'col'), may hold values from -0.1875 to 0.1875
- attn_dense: float32 [2048, 2048], P('col', 'row'), may hold values from -0.5 to 0.5
- mlp_expand: float32 [2048, 8192], P('row', 'col'), may hold values from -0.125 to 0.125
- mlp_reduce: float32 [8192, 2048], P('col', 'row'), may hold values from -0.0625 to 0.0625
- norm_params: float32 [4, 2048], replicated, may hold values from -0.4 to 1.4
- query_bias: float32 [6144], P('col'), may hold values from -0.625 to 0.625
- dense_biases: float32 [2, 2048], P(None, 'col'), may hold values from -0.625 to 0.625
- expand_bias: float32 [8192], P('col'), may hold values from -0.625 to 0.625
- norm_first: float32 [4, 2048], replicated, may hold values from -0.007954951 to 0.007954951
- norm_second: float32 [4, 2048], replicated, may hold values from 2.3071289e-06 to 0.00033325195
- query_bias_first: float32 [6144], P('col'), may hold values from -0.01171875 to 0.01171875
- query_bias_second: float32 [6144], P('col'), may hold values from 1.4404297e-05 to 5.7739257e-05
- dense_biases_first: float32 [2, 2048], P(None, 'col'), may hold values from -0.0078125 to 0.0078125
- dense_biases_second: float32 [2, 2048], P(None, 'col'), may hold values from 6.4208984e-06 to 2.5634765e-05
- expand_bias_first: float32 [8192], P('col'), may hold values from -0.001953125 to 0.001953125
- expand_bias_second: float32 [8192], P('col'), may hold values from 5.7373046e-07 to 2.3193359e-06
- query_left: float32 [16, 48, 128, 128], P('row', 'col'), may hold values from -0.0002624029 to 0.0058139654, as said below
- query_right: float32 [16, 48, 128, 128], P('row', 'col'), may hold values from -0.0002624029 to 0.0058139654, as said below
- attn_left: float32 [16, 16, 128, 128], P('col', 'row'), may hold values from -1.0496116e-05 to 0.000232683616, as said below
- attn_right: float32 [16, 16, 128, 128], P('col', 'row'), may hold values from -1.0496116e-05 to 0.000232683616, as said below
- expand_left: float32 [16, 64, 128, 128], P('row', 'col'), may hold values from -1.0496116e-05 to 0.000232683616, as said below
- expand_right: float32 [16, 64, 128, 128], P('row', 'col'), may hold values from -1.0496116e-05 to 0.000232683616, as said below
- reduce_left: float32 [64, 16, 128, 128], P('col', 'row'), may hold values from -4.1984465e-05 to 0.0009302657, as said below
- reduce_right: float32 [64, 16, 128, 128], P('col', 'row'), may hold values from -4.1984465e-05 to 0.0009302657, as said below
- query_left_root: float32 [16, 48, 128, 128], P('row', 'col'), may hold values from -0.122586672 to 1.50949655, as said below
- query_right_root: float32 [16, 48, 128, 128], P('row', 'col'), may hold values from -0.122586672 to 1.50949655, as said below
- attn_left_root: float32 [16, 16, 128, 128], P('col', 'row'), may hold values from -0.46099982 to 5.6766174, as said below
- attn_right_root: float32 [16, 16, 128, 128], P('col', 'row'), may hold values from -0.46099982 to 5.6766174, as said below
- expand_left_root: float32 [16, 64, 128, 128], P('row', 'col'), may hold values from -0.23049991 to 2.8383087, as said below
- expand_right_root: float32 [16, 64, 128, 128], P('row', 'col'), may hold values from -0.23049991 to 2.8383087, as said below
- reduce_left_root: float32 [64, 16, 128, 128], P('col', 'row'), may hold values from -0.115249955 to 1.41915435, as said below
- reduce_right_root: float32 [64, 16, 128, 128], P('col', 'row'), may hold values from -0.115249955 to 1.41915435, as said below
Outputs:
- block_out: float32 [8192, 2048], P('row', 'col')
- tokens_grad: float32 [8192, 2048], P('row', 'col')
- query_key_value_grad: float32 [2048, 6144], P('row', 'col')
- attn_dense_grad: float32 [2048, 2048], P('col', 'row')
- mlp_expand_grad: float32 [2048, 8192], P('row', 'col')
- mlp_reduce_grad: float32 [8192, 2048], P('col', 'row')
- new_query_key_value: float32 [2048, 6144], P('row', 'col')
- new_attn_dense: float32 [2048, 2048], P('col', 'row')
- new_mlp_expand: float32 [2048, 8192], P('row', 'col')
- new_mlp_reduce: float32 [8192, 2048], P('col', 'row')
- new_query_left: float32 [16, 48, 128, 128], P('row', 'col')
- new_query_right: float32 [16, 48, 128, 128], P('row', 'col')
- new_attn_left: float32 [16, 16, 128, 128], P('col', 'row')
- new_attn_right: float32 [16, 16, 128, 128], P('col', 'row')
- new_expand_left: float32 [16, 64, 128, 128], P('row', 'col')
- new_expand_right: float32 [16, 64, 128, 128], P('row', 'col')
- new_reduce_left: float32 [64, 16, 128, 128], P('col', 'row')
- new_reduce_right: float32 [64, 16, 128, 128], P('col', 'row')
- new_norm_params: float32 [4, 2048], replicated
- new_norm_first: float32 [4, 2048], replicated
- new_norm_second: float32 [4, 2048], replicated
- new_query_bias: float32 [6144], P('col')
- new_query_bias_first: float32 [6144], P('col')
- new_query_bias_second: float32 [6144], P('col')
- new_dense_biases: float32 [2, 2048], P(None, 'col')
- new_dense_biases_first: float32 [2, 2048], P(None, 'col')
- new_dense_biases_second: float32 [2, 2048], P(None, 'col')
- new_expand_bias: float32 [8192], P('col')
- new_expand_bias_first: float32 [8192], P('col')
- new_expand_bias_second: float32 [8192], P('col')
The draws below stay inside these ranges and needn't reach their ends.
Inputs may be any that keep to these rules, and one draw needn't show every extreme that they name: `sequence_lengths`: in each token block the lengths sum to 2048, nonzero ones first, zeros after. Either one sequence fills the block (in max(1, 1) blocks, drawn from the seed) or sequences of 64 to 256 tokens, multiples of 64, fill it. `query_left`: symmetric blocks. `query_right`: symmetric blocks. `attn_left`: symmetric blocks. `attn_right`: symmetric blocks. `expand_left`: symmetric blocks. `expand_right`: symmetric blocks. `reduce_left`: symmetric blocks. `reduce_right`: symmetric blocks. `query_left_root`: symmetric blocks. `query_right_root`: symmetric blocks. `attn_left_root`: symmetric blocks. `attn_right_root`: symmetric blocks. `expand_left_root`: symmetric blocks. `expand_right_root`: symmetric blocks. `reduce_left_root`: symmetric blocks. `reduce_right_root`: symmetric blocks.
All inputs are finite; a program needn't handle non-finite values.
Results may differ from the reference program's by a relative error of at most 0.012.
The reference program's roundings to bfloat16 on the way count: a program that leaves them out, or rounds other values in their place, can miss the bound.
Values may be sent and summed in bfloat16 or wider, within the bound.
A program may use at most 320 MiB of HBM per device.

```python
import math
import jax
import jax.numpy as jnp
from jax import lax

D = 2048
HEADS = 16
HD = 128
ROT = 32
FF = 8192
TOK_ROW = 2048
UNIT = 64
BLOCK = 128
GROUPS = 4
TOKENS = 8192


NORM_COEFFICIENTS = (3.6, 3.6, 0.6, 0.6)


def symmetric_noise(key, extent):
    uniform_noise = jax.random.uniform(key, extent, jnp.float32, -1.0, 1.0)
    return (uniform_noise + jnp.swapaxes(uniform_noise, -1, -2)) * (0.5 / BLOCK ** 0.5)


def statistic(key, extent, coefficient):
    magnitude = 0.05 / 0.95 * BLOCK * coefficient * coefficient / TOKENS
    diagonal = jax.random.uniform(jax.random.fold_in(key, 11), extent[:2] + (1, 1), jnp.float32, 1.5, 3.0)
    identity = jnp.eye(BLOCK, dtype=jnp.float32)
    return magnitude * (diagonal * identity + 1.6 * symmetric_noise(jax.random.fold_in(key, 12), extent))


def inverse_root(key, extent, weight_spread, coefficient):
    magnitude = (weight_spread * TOKENS ** 0.5 / coefficient) ** 0.5
    identity = jnp.eye(BLOCK, dtype=jnp.float32)
    return magnitude * (identity + symmetric_noise(jax.random.fold_in(key, 13), extent))


def query_extent():
    return (D // BLOCK, 3 * D // BLOCK, BLOCK, BLOCK)


def dense_extent():
    return (D // BLOCK, D // BLOCK, BLOCK, BLOCK)


def expand_extent():
    return (D // BLOCK, FF // BLOCK, BLOCK, BLOCK)


def reduce_extent():
    return (FF // BLOCK, D // BLOCK, BLOCK, BLOCK)


def draw_sequence_lengths(key, part):
    slot_count = TOK_ROW // UNIT
    shuffle = jax.random.permutation(jax.random.fold_in(key, 1), GROUPS)
    long_rows = shuffle < max(1, GROUPS // 4)
    unit_counts = jax.random.randint(jax.random.fold_in(key, 2), (GROUPS, slot_count), 1, 5)
    endings = jnp.cumsum(unit_counts, axis=1)
    kept_mask = endings <= slot_count
    short_rows = jnp.where(kept_mask, unit_counts, 0)
    filled = jnp.sum(kept_mask.astype(jnp.int32), axis=1, keepdims=True)
    remainder = slot_count - jnp.sum(short_rows, axis=1, keepdims=True)
    places = jnp.arange(slot_count, dtype=jnp.int32)[None, :]
    short_rows = short_rows + jnp.where(places == filled, remainder, 0)
    whole_row = jnp.where(places == 0, slot_count, 0)
    return (jnp.where(long_rows[:, None], whole_row, short_rows) * UNIT).astype(jnp.int32)


def draw_norm_params(key, part):
    gains = jax.random.uniform(jax.random.fold_in(key, 21), (2, D), jnp.float32, 0.6, 1.4)
    shifts = jax.random.uniform(jax.random.fold_in(key, 22), (2, D), jnp.float32, -0.4, 0.4)
    return jnp.stack([gains[0], shifts[0], gains[1], shifts[1]])


def draw_norm_first(key, part):
    coefficient = jnp.array(NORM_COEFFICIENTS, jnp.float32)[:, None]
    noise_draw = jax.random.uniform(jax.random.fold_in(key, 31), (4, D), jnp.float32, -1.0, 1.0)
    return 0.2 * coefficient / TOKENS ** 0.5 * noise_draw


def draw_norm_second(key, part):
    coefficient = jnp.array(NORM_COEFFICIENTS, jnp.float32)[:, None]
    factor = jax.random.uniform(jax.random.fold_in(key, 32), (4, D), jnp.float32, 1.0, 4.0)
    return 0.05 / 0.95 * coefficient * coefficient / TOKENS * factor


def draw_query_left(key, part):
    return statistic(jax.random.fold_in(key, 101), query_extent(), 1.5)


def draw_query_right(key, part):
    return statistic(jax.random.fold_in(key, 102), query_extent(), 1.5)


def draw_attn_left(key, part):
    return statistic(jax.random.fold_in(key, 103), dense_extent(), 0.3)


def draw_attn_right(key, part):
    return statistic(jax.random.fold_in(key, 104), dense_extent(), 0.3)


def draw_expand_left(key, part):
    return statistic(jax.random.fold_in(key, 105), expand_extent(), 0.3)


def draw_expand_right(key, part):
    return statistic(jax.random.fold_in(key, 106), expand_extent(), 0.3)


def draw_reduce_left(key, part):
    return statistic(jax.random.fold_in(key, 107), reduce_extent(), 0.6)


def draw_reduce_right(key, part):
    return statistic(jax.random.fold_in(key, 108), reduce_extent(), 0.6)


def draw_query_left_root(key, part):
    return inverse_root(jax.random.fold_in(key, 201), query_extent(), (D // 2) ** (-0.5), 1.5)


def draw_query_right_root(key, part):
    return inverse_root(jax.random.fold_in(key, 202), query_extent(), (D // 2) ** (-0.5), 1.5)


def draw_attn_left_root(key, part):
    return inverse_root(jax.random.fold_in(key, 203), dense_extent(), (D // 16) ** (-0.5), 0.3)


def draw_attn_right_root(key, part):
    return inverse_root(jax.random.fold_in(key, 204), dense_extent(), (D // 16) ** (-0.5), 0.3)


def draw_expand_left_root(key, part):
    return inverse_root(jax.random.fold_in(key, 205), expand_extent(), D ** (-0.5), 0.3)


def draw_expand_right_root(key, part):
    return inverse_root(jax.random.fold_in(key, 206), expand_extent(), D ** (-0.5), 0.3)


def draw_reduce_left_root(key, part):
    return inverse_root(jax.random.fold_in(key, 207), reduce_extent(), FF ** (-0.5), 0.6)


def draw_reduce_right_root(key, part):
    return inverse_root(jax.random.fold_in(key, 208), reduce_extent(), FF ** (-0.5), 0.6)


def steps_of(stream_key, dims, shards, low, largest):
    factor_of, own = 1.0, jax.random.fold_in(stream_key, 6)
    for position, blocks in shards:
        draws = jnp.exp(jax.random.uniform(jax.random.fold_in(own, position), (blocks,), jnp.float32, low / len(shards), largest / len(shards)))
        factor_of = factor_of * jnp.repeat(draws, dims[position] // blocks).reshape([-1 if axis == position else 1 for axis in range(len(dims))])
    return factor_of


def noise(own_key, shape, scale, limit, cuts=(), kind=jnp.bfloat16):
    values = jax.random.normal(own_key, shape, jnp.float32) * scale
    if len(cuts) > 0:
        values = steps_of(own_key, shape, cuts, -0.22, 0.18) * values
    return jnp.clip(values, min=-limit, max=limit).astype(kind)


def setup_inputs(seed: int = 0) -> dict:
    splits = jax.random.split(jax.random.key(seed), 37)
    return {
        "tokens_in": noise(splits[0], (TOKENS, D), 1.0, 6.0, ((0, 4), (1, 8))),
        "grad_out": noise(splits[1], (TOKENS, D), 1.0, 6.0, ((0, 4), (1, 8))),
        "sequence_lengths": draw_sequence_lengths(jax.random.fold_in(splits[36], 71), 0),
        "step_count": jax.random.randint(splits[3], (1,), 2, 21).astype(jnp.int32),
        "query_key_value": noise(splits[4], (D, 3 * D), (D // 2) ** -0.5, 0.1875, ((0, 4), (1, 8)), jnp.float32),
        "attn_dense": noise(splits[5], (D, D), (D // 16) ** -0.5, 0.5, ((0, 8), (1, 4)), jnp.float32),
        "mlp_expand": noise(splits[6], (D, FF), D ** -0.5, 0.125, ((0, 4), (1, 8)), jnp.float32),
        "mlp_reduce": noise(splits[7], (FF, D), FF ** -0.5, 0.0625, ((0, 8), (1, 4)), jnp.float32),
        "norm_params": draw_norm_params(jax.random.fold_in(splits[36], 71), 0),
        "query_bias": noise(splits[9], (3 * D,), 0.1, 0.625, ((0, 8),), jnp.float32),
        "dense_biases": noise(splits[10], (2, D), 0.1, 0.625, ((1, 8),), jnp.float32),
        "expand_bias": noise(splits[11], (FF,), 0.1, 0.625, ((0, 8),), jnp.float32),
        "norm_first": draw_norm_first(jax.random.fold_in(splits[36], 71), 0),
        "norm_second": draw_norm_second(jax.random.fold_in(splits[36], 71), 0),
        "query_bias_first": noise(splits[14], (3 * D,), (0.17 / TOKENS ** 0.5), 0.01171875, ((0, 8),), jnp.float32),
        "query_bias_second": jnp.clip(1.4404296962311491e-05 + 4.333495962782763e-05 * jax.random.uniform(splits[15], (3 * D,), jnp.float32) ** steps_of(splits[15], (3 * D,), ((0, 8),), -0.2, 0.2), 1.4404296962311491e-05, 5.773925659013912e-05),
        "dense_biases_first": noise(splits[16], (2, D), (0.111 / TOKENS ** 0.5), 0.0078125, ((1, 8),), jnp.float32),
        "dense_biases_second": jnp.clip(6.420898444048362e-06 + 1.92138663805963e-05 * jax.random.uniform(splits[17], (2, D), jnp.float32) ** steps_of(splits[17], (2, D), ((1, 8),), -0.2, 0.2), 6.420898444048362e-06, 2.5634764824644662e-05),
        "expand_bias_first": noise(splits[18], (FF,), (0.033 / TOKENS ** 0.5), 0.001953125, ((0, 8),), jnp.float32),
        "expand_bias_second": jnp.clip(5.737304604735982e-07 + 1.7456054024478362e-06 * jax.random.uniform(splits[19], (FF,), jnp.float32) ** steps_of(splits[19], (FF,), ((0, 8),), -0.2, 0.2), 5.737304604735982e-07, 2.3193358629214345e-06),
        "query_left": draw_query_left(jax.random.fold_in(splits[36], 71), 0),
        "query_right": draw_query_right(jax.random.fold_in(splits[36], 71), 0),
        "attn_left": draw_attn_left(jax.random.fold_in(splits[36], 71), 0),
        "attn_right": draw_attn_right(jax.random.fold_in(splits[36], 71), 0),
        "expand_left": draw_expand_left(jax.random.fold_in(splits[36], 71), 0),
        "expand_right": draw_expand_right(jax.random.fold_in(splits[36], 71), 0),
        "reduce_left": draw_reduce_left(jax.random.fold_in(splits[36], 71), 0),
        "reduce_right": draw_reduce_right(jax.random.fold_in(splits[36], 71), 0),
        "query_left_root": draw_query_left_root(jax.random.fold_in(splits[36], 71), 0),
        "query_right_root": draw_query_right_root(jax.random.fold_in(splits[36], 71), 0),
        "attn_left_root": draw_attn_left_root(jax.random.fold_in(splits[36], 71), 0),
        "attn_right_root": draw_attn_right_root(jax.random.fold_in(splits[36], 71), 0),
        "expand_left_root": draw_expand_left_root(jax.random.fold_in(splits[36], 71), 0),
        "expand_right_root": draw_expand_right_root(jax.random.fold_in(splits[36], 71), 0),
        "reduce_left_root": draw_reduce_left_root(jax.random.fold_in(splits[36], 71), 0),
        "reduce_right_root": draw_reduce_right_root(jax.random.fold_in(splits[36], 71), 0),
    }


NORM_EPS = 1e-05
ROPE_BASE = 10000.0
MASKED = -1e+30
PRECISE = lax.Precision.HIGHEST
SHAMPOO_DECAY = 0.95
MATRIX_RATE = 0.5
WEIGHT_DECAY = 0.01
FIRST_DECAY = 0.9
SECOND_DECAY = 0.95
VECTOR_RATE = 0.6
ADAM_EPS = 1e-08

@jax.custom_vjp
def low(v):
    return lax.optimization_barrier(v.astype(jnp.bfloat16)).astype(jnp.float32)

@jax.custom_vjp
def low_back(v):
    return v

def low_keep(v):
    return (low(v), None)

def low_pass(kept, grad):
    return (grad,)

def back_keep(v):
    return (v, None)

def back_low(kept, grad):
    return (low(grad),)
low.defvjp(low_keep, low_pass)
low_back.defvjp(back_keep, back_low)

def product(first_factor, second_factor):
    return jnp.dot(first_factor, second_factor, precision=PRECISE, preferred_element_type=jnp.float32)

def layer_norm(values, gain_row, shift_row):
    center = values - lax.optimization_barrier(jnp.mean(values, -1, keepdims=True))
    spread = lax.optimization_barrier(jnp.mean(center * center, -1, keepdims=True))
    return center * lax.rsqrt(spread + NORM_EPS) * gain_row + shift_row

def positions(lengths):
    tokens = jnp.arange(TOK_ROW, dtype=jnp.int32)
    endings = jnp.cumsum(lengths, dtype=jnp.int32)
    finished = (endings[None, :] <= tokens[:, None]).astype(jnp.int32)
    segment = lax.optimization_barrier(jnp.sum(finished, -1, dtype=jnp.int32))
    offset = lax.optimization_barrier(jnp.sum(finished * lengths[None, :], -1, dtype=jnp.int32))
    return (segment, tokens - offset)

def rotary_tables(places):
    middle = ROT // 2
    indices = jnp.arange(middle, dtype=jnp.float32)
    inverse = jnp.exp(indices * (-2.0 * math.log(ROPE_BASE) / ROT))
    angles = places.astype(jnp.float32)[:, None] * inverse[None, :]
    angles = jnp.concatenate([angles, angles], -1)
    return (jnp.cos(angles), jnp.sin(angles))

def rotate(vectors, cosine_table, sine_table):
    middle = ROT // 2
    turning = vectors[..., :ROT]
    swapped = jnp.concatenate([-turning[..., middle:], turning[..., :middle]], -1)
    return jnp.concatenate([turning * cosine_table + swapped * sine_table, vectors[..., ROT:]], -1)

def attend_one(items):
    triple, segment, places = items
    cosine_table, sine_table = rotary_tables(places)
    queries = low(rotate(triple[:, 0], cosine_table, sine_table))
    key_rows = low(rotate(triple[:, 1], cosine_table, sine_table))
    value_rows = low(triple[:, 2])
    raw_scores = low_back(product(queries, key_rows.T))
    tokens = jnp.arange(TOK_ROW, dtype=jnp.int32)
    allowed = (segment[:, None] == segment[None, :]) & (tokens[:, None] >= tokens[None, :])
    scores = jnp.where(allowed, raw_scores * HD ** (-0.5), MASKED)
    attn_weights = low(jax.nn.softmax(scores, axis=-1))
    return product(attn_weights, value_rows)

def shampoo(weight, gradient, left_stat, right_stat, left_root, right_root, scaling):
    height, breadth = gradient.shape
    blocksize = left_stat.shape[-1]
    mean_grad = gradient * scaling
    pieces = mean_grad.reshape(height // blocksize, blocksize, breadth // blocksize, blocksize).transpose(0, 2, 1, 3)
    new_left = SHAMPOO_DECAY * left_stat + (1.0 - SHAMPOO_DECAY) * jnp.einsum('ijab,ijcb->ijac', pieces, pieces, precision=PRECISE)
    new_right = SHAMPOO_DECAY * right_stat + (1.0 - SHAMPOO_DECAY) * jnp.einsum('ijba,ijbc->ijac', pieces, pieces, precision=PRECISE)
    turned = jnp.einsum('ijab,ijbc->ijac', left_root, pieces, precision=PRECISE)
    turned = jnp.einsum('ijab,ijbc->ijac', turned, right_root, precision=PRECISE)
    update = turned.transpose(0, 2, 1, 3).reshape(height, breadth)
    new_weight = weight - MATRIX_RATE * (update + WEIGHT_DECAY * weight)
    return (new_weight, new_left, new_right)

def adam(vector, moment_one, moment_two, gradient, scaling, counter):
    mean_grad = gradient * scaling
    new_one = FIRST_DECAY * moment_one + (1.0 - FIRST_DECAY) * mean_grad
    new_two = SECOND_DECAY * moment_two + (1.0 - SECOND_DECAY) * mean_grad * mean_grad
    first_hat = new_one / (1.0 - FIRST_DECAY ** counter)
    second_hat = new_two / (1.0 - SECOND_DECAY ** counter)
    new_vector = vector - VECTOR_RATE * first_hat / (jnp.sqrt(second_hat) + ADAM_EPS)
    return (new_vector, new_one, new_two)

def reference(tokens_in, grad_out, sequence_lengths, step_count, query_key_value, attn_dense, mlp_expand, mlp_reduce, norm_params, query_bias, dense_biases, expand_bias, norm_first, norm_second, query_bias_first, query_bias_second, dense_biases_first, dense_biases_second, expand_bias_first, expand_bias_second, query_left, query_right, attn_left, attn_right, expand_left, expand_right, reduce_left, reduce_right, query_left_root, query_right_root, attn_left_root, attn_right_root, expand_left_root, expand_right_root, reduce_left_root, reduce_right_root):
    segments, places = jax.vmap(positions)(sequence_lengths)
    segment_heads = jnp.repeat(segments, HEADS, axis=0)
    place_heads = jnp.repeat(places, HEADS, axis=0)

    def layer(inputs, triple_weight, dense_weight, expand_weight, reduce_weight, gains_shifts, triple_bias, dense_shifts, expand_shift):
        first_in = low(layer_norm(inputs, gains_shifts[0], gains_shifts[1]))
        second_in = low(layer_norm(inputs, gains_shifts[2], gains_shifts[3]))
        triple = low_back(product(first_in, low(triple_weight)) + triple_bias)
        triple = triple.reshape(GROUPS, TOK_ROW, HEADS, 3, HD).transpose(0, 2, 1, 3, 4).reshape(GROUPS * HEADS, TOK_ROW, 3, HD)
        outputs = lax.map(jax.checkpoint(attend_one), (triple, segment_heads, place_heads))
        attended = outputs.reshape(GROUPS, HEADS, TOK_ROW, HD).transpose(0, 2, 1, 3).reshape(TOKENS, D)
        attended = low(low_back(attended))
        hidden = low_back(product(second_in, low(expand_weight)) + expand_shift)
        activated = low(jax.nn.gelu(hidden, approximate=False))
        attn_branch = product(attended, low(dense_weight)) + dense_shifts[0]
        mlp_branch = product(activated, low(reduce_weight)) + dense_shifts[1]
        return inputs + attn_branch + mlp_branch
    block_out, pullback = jax.vjp(layer, tokens_in.astype(jnp.float32), query_key_value, attn_dense, mlp_expand, mlp_reduce, norm_params, query_bias, dense_biases, expand_bias)
    grads = pullback(grad_out.astype(jnp.float32))
    tokens_grad = grads[0]
    scaling = 1.0 / TOKENS
    counter = step_count[0].astype(jnp.float32)
    new_qkv, new_query_left, new_query_right = shampoo(query_key_value, grads[1], query_left, query_right, query_left_root, query_right_root, scaling)
    new_dense, new_attn_left, new_attn_right = shampoo(attn_dense, grads[2], attn_left, attn_right, attn_left_root, attn_right_root, scaling)
    new_expand, new_expand_left, new_expand_right = shampoo(mlp_expand, grads[3], expand_left, expand_right, expand_left_root, expand_right_root, scaling)
    new_reduce, new_reduce_left, new_reduce_right = shampoo(mlp_reduce, grads[4], reduce_left, reduce_right, reduce_left_root, reduce_right_root, scaling)
    new_norm, new_norm_one, new_norm_two = adam(norm_params, norm_first, norm_second, grads[5], scaling, counter)
    new_qbias, new_qbias_one, new_qbias_two = adam(query_bias, query_bias_first, query_bias_second, grads[6], scaling, counter)
    new_dbias, new_dbias_one, new_dbias_two = adam(dense_biases, dense_biases_first, dense_biases_second, grads[7], scaling, counter)
    new_ebias, new_ebias_one, new_ebias_two = adam(expand_bias, expand_bias_first, expand_bias_second, grads[8], scaling, counter)
    return (block_out, tokens_grad, grads[1], grads[2], grads[3], grads[4], new_qkv, new_dense, new_expand, new_reduce, new_query_left, new_query_right, new_attn_left, new_attn_right, new_expand_left, new_expand_right, new_reduce_left, new_reduce_right, new_norm, new_norm_one, new_norm_two, new_qbias, new_qbias_one, new_qbias_two, new_dbias, new_dbias_one, new_dbias_two, new_ebias, new_ebias_one, new_ebias_two)
```

```python
import functools
import math

import jax
import jax.numpy as jnp
from jax import lax
from jax.experimental import pallas as pl
from jax.experimental.pallas import tpu as pltpu
from jax.sharding import PartitionSpec as P


HD = 128
ROT = 32


NORM_EPS = 1e-05
ROPE_BASE = 10000.0
MASKED = -1e30
SHAMPOO_DECAY = 0.95
MATRIX_RATE = 0.5
WEIGHT_DECAY = 0.01
FIRST_DECAY = 0.9
SECOND_DECAY = 0.95
VECTOR_RATE = 0.6
ADAM_EPS = 1e-08

NT = (((1,), (1,)), ((), ()))
TN = (((0,), (0,)), ((), ()))
NN = (((1,), (0,)), ((), ()))
VMEM_BYTES = 60 * 1024 * 1024


def mm(a, b, dims=NN):
    return lax.dot_general(a, b, dims, preferred_element_type=jnp.float32)


def params(*semantics):
    return pltpu.CompilerParams(dimension_semantics=semantics, vmem_limit_bytes=VMEM_BYTES)


def cost(flops, moved, exps=0):
    return pl.CostEstimate(flops=int(flops), bytes_accessed=int(moved), transcendentals=int(exps))


def whole(shape):
    return pl.BlockSpec(
        shape, lambda *_: (0,) * len(shape), pipeline_mode=pl.Buffered(buffer_count=1)
    )


def positions(lengths, number):
    tokens = jnp.arange(number, dtype=jnp.int32)
    endings = jnp.cumsum(lengths, dtype=jnp.int32)
    finished = (endings[None, :] <= tokens[:, None]).astype(jnp.int32)
    return jnp.sum(finished * lengths[None, :], -1, dtype=jnp.int32)


def rotary_tables(places):
    middle = ROT // 2
    indices = jnp.arange(middle, dtype=jnp.float32)
    inverse = jnp.exp(indices * (-2.0 * math.log(ROPE_BASE) / ROT))
    angles = places.astype(jnp.float32)[:, None] * inverse[None, :]
    cosine, sine = jnp.cos(angles), jnp.sin(angles)
    number = places.shape[0]
    ones = jnp.ones((number, HD - ROT), jnp.float32)
    gap = jnp.zeros((number, middle), jnp.float32)
    rest = jnp.zeros((number, HD - ROT), jnp.float32)
    return (
        jnp.concatenate([cosine, cosine, ones], -1),
        jnp.concatenate([-sine, gap, rest], -1),
        jnp.concatenate([gap, sine, rest], -1),
    )


def turn(vectors, own, ahead, behind):
    middle = ROT // 2
    return (
        vectors * own
        + pltpu.roll(vectors, HD - middle, 1) * ahead
        + pltpu.roll(vectors, middle, 1) * behind
    )


def front_kernel(
    x_ref, norm_ref, wq_ref, qb_ref, own_ref, ahead_ref, behind_ref, we_ref, eb_ref,
    one_ref, two_ref, stat_ref, qkv_ref, act_ref, slope_ref,
):
    x = x_ref[...].astype(jnp.float32)
    mu = jnp.mean(x, -1, keepdims=True)
    center = x - mu
    inverse = lax.rsqrt(jnp.mean(center * center, -1, keepdims=True) + NORM_EPS)
    normalized = center * inverse
    stat_ref[...] = jnp.concatenate([mu, inverse], -1)
    one = (normalized * norm_ref[0:1] + norm_ref[1:2]).astype(jnp.bfloat16)
    two = (normalized * norm_ref[2:3] + norm_ref[3:4]).astype(jnp.bfloat16)
    one_ref[...] = one
    two_ref[...] = two
    own, ahead, behind = own_ref[...], ahead_ref[...], behind_ref[...]
    for head in range(wq_ref.shape[1] // (3 * HD)):
        cols = slice(head * 3 * HD, (head + 1) * 3 * HD)
        triple = mm(one, wq_ref[:, cols]) + qb_ref[:, cols]
        query = turn(triple[:, :HD], own, ahead, behind)
        key = turn(triple[:, HD : 2 * HD], own, ahead, behind)
        qkv_ref[:, cols] = jnp.concatenate([query, key, triple[:, 2 * HD :]], -1).astype(
            jnp.bfloat16
        )
    width = 256
    for first in range(0, we_ref.shape[1], width):
        cols = slice(first, first + width)
        hidden = mm(two, we_ref[:, cols]) + eb_ref[:, cols]
        phi = 0.5 + 0.5 * lax.erf(hidden * (0.5**0.5))
        act_ref[:, cols] = (hidden * phi).astype(jnp.bfloat16)
        density = jnp.exp(-0.5 * hidden * hidden) * ((0.5 / math.pi) ** 0.5)
        slope_ref[:, cols] = phi + hidden * density


def front(panel, norm_params, wq, qbias, tables, we, ebias):
    tokens, features = panel.shape
    tile = 256
    wide, hidden = wq.shape[1], we.shape[1]

    def rows(width):
        return pl.BlockSpec((tile, width), lambda i: (i, 0))

    return pl.pallas_call(
        front_kernel,
        grid=(tokens // tile,),
        in_specs=[
            rows(features),
            whole(norm_params.shape),
            whole(wq.shape),
            whole((1, wide)),
            rows(HD),
            rows(HD),
            rows(HD),
            whole(we.shape),
            whole((1, hidden)),
        ],
        out_specs=[rows(features), rows(features), rows(2), rows(wide), rows(hidden), rows(hidden)],
        out_shape=[
            jax.ShapeDtypeStruct((tokens, features), jnp.bfloat16),
            jax.ShapeDtypeStruct((tokens, features), jnp.bfloat16),
            jax.ShapeDtypeStruct((tokens, 2), jnp.float32),
            jax.ShapeDtypeStruct((tokens, wide), jnp.bfloat16),
            jax.ShapeDtypeStruct((tokens, hidden), jnp.bfloat16),
            jax.ShapeDtypeStruct((tokens, hidden), jnp.float32),
        ],
        compiler_params=params("arbitrary"),
        cost_estimate=cost(
            2 * tokens * features * (wide + hidden), tokens * (6 * features + 2 * wide + 6 * hidden)
        ),
        name="front",
    )(panel, norm_params, wq, qbias[None], *tables, we, ebias[None])


def scores(q, k, first, rows, begin, start):
    raw = mm(q, k, NT) * HD**-0.5
    cols = start + lax.broadcasted_iota(jnp.int32, raw.shape, 1)
    return raw, (cols >= begin) & (cols <= rows)


def attend_kernel(from_ref, q_ref, k_ref, v_ref, begin_ref, out_ref, sum_ref, held):
    tile, span = q_ref.shape[0], held.shape[2]
    block = pl.program_id(1)
    low, high = from_ref[block], (block * tile + tile - 1) // span + 1
    q, begin = q_ref[...], begin_ref[...]
    rows = block * tile + lax.broadcasted_iota(jnp.int32, (tile, 1), 0)

    def first_pass(j, top):
        start = pl.multiple_of(j * span, span)
        raw, allowed = scores(q, k_ref[pl.ds(start, span)], block, rows, begin, start)
        raw = jnp.where(allowed, raw, MASKED)
        held[j] = raw
        return jnp.maximum(top, jnp.max(raw, -1, keepdims=True))

    top = lax.fori_loop(low, high, first_pass, jnp.full((tile, 1), MASKED, jnp.float32))

    def second_pass(j, carry):
        total, out = carry
        start = pl.multiple_of(j * span, span)
        weights = jnp.exp(held[j] - top)
        total = total + jnp.sum(weights, -1, keepdims=True)
        return total, out + mm(weights.astype(jnp.bfloat16), v_ref[pl.ds(start, span)])

    total, out = lax.fori_loop(
        low,
        high,
        second_pass,
        (jnp.zeros((tile, 1), jnp.float32), jnp.zeros((tile, HD), jnp.float32)),
    )
    out_ref[...] = (out / total).astype(jnp.bfloat16)
    sum_ref[...] = top + jnp.log(total)


def tiles(length):
    return min(256, length), min(512, length)


def attend(qkv, begin):
    length = qkv.shape[0]
    heads = qkv.shape[1] // (3 * HD)
    tile, span = tiles(length)
    grid_spec = pltpu.PrefetchScalarGridSpec(
        num_scalar_prefetch=1,
        grid=(heads, length // tile),
        in_specs=[
            pl.BlockSpec((tile, HD), lambda h, i, _: (i, 3 * h)),
            pl.BlockSpec((length, HD), lambda h, i, _: (0, 3 * h + 1)),
            pl.BlockSpec((length, HD), lambda h, i, _: (0, 3 * h + 2)),
            pl.BlockSpec((tile, 1), lambda h, i, _: (i, 0)),
        ],
        out_specs=[
            pl.BlockSpec((tile, HD), lambda h, i, _: (i, h)),
            pl.BlockSpec((None, tile, 1), lambda h, i, _: (h, i, 0)),
        ],
        scratch_shapes=[pltpu.VMEM((length // span, tile, span), jnp.float32)],
    )
    return pl.pallas_call(
        attend_kernel,
        grid_spec=grid_spec,
        out_shape=[
            jax.ShapeDtypeStruct((length, heads * HD), jnp.bfloat16),
            jax.ShapeDtypeStruct((heads, length, 1), jnp.float32),
        ],
        compiler_params=params("arbitrary", "arbitrary"),
        cost_estimate=cost(4 * heads * length * length * HD, 8 * heads * length * HD, heads * length * length),
        name="attend",
    )(begin[::tile] // span, qkv, qkv, qkv, begin[:, None])


def attend_back_kernel(
    from_ref, q_ref, k_ref, v_ref, grad_ref, begin_ref, sum_ref, own_ref, ahead_ref, behind_ref,
    out_ref, probs, probs_back, key_back, value_back,
):
    tile, span = q_ref.shape[0], probs.shape[2]
    block, blocks = pl.program_id(1), pl.num_programs(1)
    low, high = from_ref[block], (block * tile + tile - 1) // span + 1
    q, grad, begin, logsum = q_ref[...], grad_ref[...], begin_ref[...], sum_ref[...]
    rows = block * tile + lax.broadcasted_iota(jnp.int32, (tile, 1), 0)

    @pl.when(block == 0)
    def _():
        key_back[...] = jnp.zeros_like(key_back)
        value_back[...] = jnp.zeros_like(value_back)

    def first_pass(j, inner):
        start = pl.multiple_of(j * span, span)
        raw, allowed = scores(q, k_ref[pl.ds(start, span)], block, rows, begin, start)
        weights = jnp.where(allowed, jnp.exp(raw - logsum), 0.0)
        back = mm(grad, v_ref[pl.ds(start, span)], NT)
        probs[j] = weights
        probs_back[j] = back
        return inner + jnp.sum(weights * back, -1, keepdims=True)

    inner = lax.fori_loop(low, high, first_pass, jnp.zeros((tile, 1), jnp.float32))

    def second_pass(j, query_back):
        start = pl.multiple_of(j * span, span)
        weights = probs[j]
        raw_back = (weights * (probs_back[j] - inner) * HD**-0.5).astype(jnp.bfloat16)
        part = pl.ds(start, span)
        key_back[part] += mm(raw_back, q, TN)
        value_back[part] += mm(weights.astype(jnp.bfloat16), grad, TN)
        return query_back + mm(raw_back, k_ref[part])

    query_back = lax.fori_loop(low, high, second_pass, jnp.zeros((tile, HD), jnp.float32))
    here = pl.ds(pl.multiple_of(block * tile, tile), tile)
    query_back = turn(query_back, own_ref[here], -ahead_ref[here], -behind_ref[here])
    out_ref[here, :HD] = query_back.astype(jnp.bfloat16)

    @pl.when(block == blocks - 1)
    def _():
        def finish(i, _):
            at = pl.ds(pl.multiple_of(i * tile, tile), tile)
            keys = turn(key_back[at], own_ref[at], -ahead_ref[at], -behind_ref[at])
            out_ref[at, HD : 2 * HD] = keys.astype(jnp.bfloat16)
            out_ref[at, 2 * HD :] = value_back[at].astype(jnp.bfloat16)
            return 0

        lax.fori_loop(0, blocks, finish, 0)


def attend_back(qkv, begin, grad, logsum, tables):
    length = qkv.shape[0]
    heads = qkv.shape[1] // (3 * HD)
    tile, span = tiles(length)
    grid_spec = pltpu.PrefetchScalarGridSpec(
        num_scalar_prefetch=1,
        grid=(heads, length // tile),
        in_specs=[
            pl.BlockSpec((tile, HD), lambda h, i, _: (i, 3 * h)),
            pl.BlockSpec((length, HD), lambda h, i, _: (0, 3 * h + 1)),
            pl.BlockSpec((length, HD), lambda h, i, _: (0, 3 * h + 2)),
            pl.BlockSpec((tile, HD), lambda h, i, _: (i, h)),
            pl.BlockSpec((tile, 1), lambda h, i, _: (i, 0)),
            pl.BlockSpec((None, tile, 1), lambda h, i, _: (h, i, 0)),
            whole((length, HD)),
            whole((length, HD)),
            whole((length, HD)),
        ],
        out_specs=[pl.BlockSpec((length, 3 * HD), lambda h, i, _: (0, h))],
        scratch_shapes=[
            pltpu.VMEM((length // span, tile, span), jnp.float32),
            pltpu.VMEM((length // span, tile, span), jnp.float32),
            pltpu.VMEM((length, HD), jnp.float32),
            pltpu.VMEM((length, HD), jnp.float32),
        ],
    )
    return pl.pallas_call(
        attend_back_kernel,
        grid_spec=grid_spec,
        out_shape=[jax.ShapeDtypeStruct(qkv.shape, jnp.bfloat16)],
        compiler_params=params("arbitrary", "arbitrary"),
        cost_estimate=cost(10 * heads * length * length * HD, 14 * heads * length * HD, heads * length * length),
        name="attend_back",
    )(begin[::tile] // span, qkv, qkv, qkv, grad, begin[:, None], logsum, *tables)[0]


def join_kernel(a_ref, wa_ref, b_ref, wb_ref, out_ref):
    out_ref[...] = (mm(a_ref[...], wa_ref[...]) + mm(b_ref[...], wb_ref[...])).astype(out_ref.dtype)


def join(a, wa, b, wb):
    tokens, features = a.shape[0], wa.shape[1]
    tile = 256
    return pl.pallas_call(
        join_kernel,
        grid=(tokens // tile,),
        in_specs=[
            pl.BlockSpec((tile, a.shape[1]), lambda i: (i, 0)),
            whole(wa.shape),
            pl.BlockSpec((tile, b.shape[1]), lambda i: (i, 0)),
            whole(wb.shape),
        ],
        out_specs=pl.BlockSpec((tile, features), lambda i: (i, 0)),
        out_shape=jax.ShapeDtypeStruct((tokens, features), jnp.bfloat16),
        compiler_params=params("arbitrary"),
        cost_estimate=cost(2 * tokens * features * (a.shape[1] + b.shape[1]), 4 * tokens * features),
        name="join",
    )(a, wa, b, wb)


def part_kernel(g_ref, wd_ref, wr_ref, slope_ref, att_ref, hid_ref, sum_ref):
    g = g_ref[...]
    att_ref[...] = mm(g, wd_ref[...], NT).astype(jnp.bfloat16)

    @pl.when(pl.program_id(0) == 0)
    def _():
        sum_ref[...] = jnp.zeros_like(sum_ref)

    width = 256
    for first in range(0, wr_ref.shape[0], width):
        cols = slice(first, first + width)
        back = (mm(g, wr_ref[cols], NT) * slope_ref[:, cols]).astype(jnp.bfloat16)
        hid_ref[:, cols] = back
        sum_ref[:, cols] += jnp.sum(back.astype(jnp.float32), 0, keepdims=True)


def part(g, wd, wr, slope):
    tokens, features = g.shape
    tile = 256

    def rows(width):
        return pl.BlockSpec((tile, width), lambda i: (i, 0))

    return pl.pallas_call(
        part_kernel,
        grid=(tokens // tile,),
        in_specs=[rows(features), whole(wd.shape), whole(wr.shape), rows(wr.shape[0])],
        out_specs=[
            rows(wd.shape[0]),
            rows(wr.shape[0]),
            pl.BlockSpec((1, wr.shape[0]), lambda i: (0, 0)),
        ],
        out_shape=[
            jax.ShapeDtypeStruct((tokens, wd.shape[0]), jnp.bfloat16),
            jax.ShapeDtypeStruct((tokens, wr.shape[0]), jnp.bfloat16),
            jax.ShapeDtypeStruct((1, wr.shape[0]), jnp.float32),
        ],
        compiler_params=params("arbitrary"),
        cost_estimate=cost(
            2 * tokens * features * (wd.shape[0] + wr.shape[0]), tokens * (2 * features + 8 * wr.shape[0])
        ),
        name="part",
    )(g, wd, wr, slope)


def back_kernel(tb_ref, wq_ref, hb_ref, we_ref, x_ref, stat_ref, norm_ref, out_ref, row_ref, col_ref):
    @pl.when(pl.program_id(0) == 0)
    def _():
        col_ref[...] = jnp.zeros_like(col_ref)

    triple_back, hidden_back = tb_ref[...], hb_ref[...]
    mu, inverse = stat_ref[:, 0:1], stat_ref[:, 1:2]
    width = 256
    plain = jnp.zeros((tb_ref.shape[0], 1), jnp.float32)
    crossed = plain
    for first in range(0, x_ref.shape[1], width):
        cols = slice(first, first + width)
        one = mm(triple_back, wq_ref[cols], NT)
        two = mm(hidden_back, we_ref[cols], NT)
        normalized = (x_ref[:, cols].astype(jnp.float32) - mu) * inverse
        col_ref[:, cols] += jnp.concatenate(
            [
                jnp.sum(one * normalized, 0, keepdims=True),
                jnp.sum(one, 0, keepdims=True),
                jnp.sum(two * normalized, 0, keepdims=True),
                jnp.sum(two, 0, keepdims=True),
            ],
            0,
        )
        both = one * norm_ref[0:1, cols] + two * norm_ref[2:3, cols]
        out_ref[:, cols] = both.astype(jnp.bfloat16)
        plain = plain + jnp.sum(both, -1, keepdims=True)
        crossed = crossed + jnp.sum(both * normalized, -1, keepdims=True)
    row_ref[...] = jnp.concatenate([plain, crossed], -1)


def back(triple_back, wq, hidden_back, we, panel, stats, norm_params):
    tokens, features = panel.shape
    tile = 256

    def rows(width):
        return pl.BlockSpec((tile, width), lambda i: (i, 0))

    return pl.pallas_call(
        back_kernel,
        grid=(tokens // tile,),
        in_specs=[
            rows(wq.shape[1]),
            whole(wq.shape),
            rows(we.shape[1]),
            whole(we.shape),
            rows(features),
            rows(2),
            whole(norm_params.shape),
        ],
        out_specs=[rows(features), rows(2), pl.BlockSpec((4, features), lambda i: (0, 0))],
        out_shape=[
            jax.ShapeDtypeStruct((tokens, features), jnp.bfloat16),
            jax.ShapeDtypeStruct((tokens, 2), jnp.float32),
            jax.ShapeDtypeStruct((4, features), jnp.float32),
        ],
        compiler_params=params("arbitrary"),
        cost_estimate=cost(
            2 * tokens * features * (wq.shape[1] + we.shape[1]), tokens * 6 * features
        ),
        name="back",
    )(triple_back, wq, hidden_back, we, panel, stats, norm_params)


def shampoo_kernel(scaling, w_ref, g_ref, l_ref, r_ref, p_ref, q_ref, nw_ref, nl_ref, nr_ref):
    size = l_ref.shape[-1]
    for block in range(l_ref.shape[1]):
        cols = slice(block * size, (block + 1) * size)
        grad = (g_ref[:, cols] * scaling).astype(jnp.bfloat16)
        nl_ref[0, block] = SHAMPOO_DECAY * l_ref[0, block] + (1.0 - SHAMPOO_DECAY) * mm(grad, grad, NT)
        nr_ref[0, block] = SHAMPOO_DECAY * r_ref[0, block] + (1.0 - SHAMPOO_DECAY) * mm(grad, grad, TN)
        turned = mm(p_ref[0, block].astype(jnp.bfloat16), grad).astype(jnp.bfloat16)
        step = mm(turned, q_ref[0, block].astype(jnp.bfloat16))
        weight = w_ref[:, cols]
        nw_ref[:, cols] = weight - MATRIX_RATE * (step + WEIGHT_DECAY * weight)


def shampoo(weight, gradient, left_stat, right_stat, left_root, right_root, scaling):
    height, breadth = gradient.shape
    size = left_stat.shape[-1]
    across = breadth // size
    flat = pl.BlockSpec((size, breadth), lambda i: (i, 0))
    cube = pl.BlockSpec((1, across, size, size), lambda i: (i, 0, 0, 0))
    return pl.pallas_call(
        functools.partial(shampoo_kernel, scaling),
        grid=(height // size,),
        in_specs=[flat, flat, cube, cube, cube, cube],
        out_specs=[flat, cube, cube],
        out_shape=[
            jax.ShapeDtypeStruct(weight.shape, jnp.float32),
            jax.ShapeDtypeStruct(left_stat.shape, jnp.float32),
            jax.ShapeDtypeStruct(right_stat.shape, jnp.float32),
        ],
        compiler_params=params("arbitrary"),
        cost_estimate=cost(8 * height * breadth * size, 36 * height * breadth),
        name="shampoo",
    )(weight, gradient, left_stat, right_stat, left_root, right_root)


def swap(value, axis, bit):
    size = lax.axis_size(axis)
    return lax.ppermute(value, axis, [(i, i ^ bit) for i in range(size)])


def gather_row(shard, dim):
    if lax.axis_size("row") != 4:
        return lax.all_gather(shard, "row", axis=dim, tiled=True)
    me = lax.axis_index("row")
    across = swap(shard, "row", 2)
    beside = swap(shard, "row", 1)
    corner = swap(across, "row", 1)
    shape = list(shard.shape)
    step = shape[dim]
    shape[dim] *= 4
    out = jnp.zeros(shape, shard.dtype)
    for bit, piece in ((0, shard), (2, across), (1, beside), (3, corner)):
        out = lax.dynamic_update_slice_in_dim(out, piece, (me ^ bit) * step, dim)
    return out


def scatter_row(value, dim):
    if lax.axis_size("row") != 4:
        return lax.psum_scatter(value, "row", scatter_dimension=dim, tiled=True)
    me = lax.axis_index("row")
    step = value.shape[dim] // 4

    def share(owner):
        return lax.dynamic_slice_in_dim(value, owner * step, step, dim)

    far_beside = swap(share(me ^ 3).astype(jnp.bfloat16), "row", 1)
    near_beside = swap(share(me ^ 1).astype(jnp.bfloat16), "row", 1)
    far = share(me ^ 2) + far_beside.astype(jnp.float32)
    across = swap(far.astype(jnp.bfloat16), "row", 2)
    return share(me) + near_beside.astype(jnp.float32) + across.astype(jnp.float32)


def total(value, axes):
    if lax.axis_size("row") != 4 or lax.axis_size("col") != 8:
        return lax.psum(value, axes)
    for axis in axes:
        bit = 1
        while bit < lax.axis_size(axis):
            value = value + swap(value, axis, bit)
            bit *= 2
    return value


def adam(vector, moment_one, moment_two, gradient, scaling, counter):
    mean_grad = gradient * scaling
    new_one = FIRST_DECAY * moment_one + (1.0 - FIRST_DECAY) * mean_grad
    new_two = SECOND_DECAY * moment_two + (1.0 - SECOND_DECAY) * mean_grad * mean_grad
    first_hat = new_one / (1.0 - FIRST_DECAY**counter)
    second_hat = new_two / (1.0 - SECOND_DECAY**counter)
    new_vector = vector - VECTOR_RATE * first_hat / (jnp.sqrt(second_hat) + ADAM_EPS)
    return (new_vector, new_one, new_two)


def local(
    tokens_in,
    grad_out,
    sequence_lengths,
    step_count,
    query_key_value,
    attn_dense,
    mlp_expand,
    mlp_reduce,
    norm_params,
    query_bias,
    dense_biases,
    expand_bias,
    norm_first,
    norm_second,
    query_bias_first,
    query_bias_second,
    dense_biases_first,
    dense_biases_second,
    expand_bias_first,
    expand_bias_second,
    query_left,
    query_right,
    attn_left,
    attn_right,
    expand_left,
    expand_right,
    reduce_left,
    reduce_right,
    query_left_root,
    query_right_root,
    attn_left_root,
    attn_right_root,
    expand_left_root,
    expand_right_root,
    reduce_left_root,
    reduce_right_root,
):
    input_panel = lax.all_gather(tokens_in, "col", axis=1, tiled=True)
    query_full = gather_row(query_key_value.astype(jnp.bfloat16), 0)
    expand_full = gather_row(mlp_expand.astype(jnp.bfloat16), 0)
    dense_full = gather_row(attn_dense.astype(jnp.bfloat16), 1)
    reduce_full = gather_row(mlp_reduce.astype(jnp.bfloat16), 1)
    cotangent_panel = lax.all_gather(grad_out, "col", axis=1, tiled=True)
    row_count, col_width = tokens_in.shape
    features = input_panel.shape[1]
    col_start = lax.axis_index("col") * col_width
    begin = positions(sequence_lengths[0], row_count)
    tables = rotary_tables(jnp.arange(row_count, dtype=jnp.int32) - begin)
    first_in, second_in, stats, qkv, activated, slope = front(
        input_panel, norm_params, query_full, query_bias, tables, expand_full, expand_bias
    )
    attended, logsum = attend(qkv, begin)
    branches = join(attended, dense_full, activated, reduce_full)
    branch_share = lax.psum_scatter(branches, "col", scatter_dimension=1, tiled=True)
    block_out = (
        tokens_in.astype(jnp.float32)
        + branch_share.astype(jnp.float32)
        + dense_biases[0]
        + dense_biases[1]
    )
    attended_back, hidden_back, hidden_sum = part(cotangent_panel, dense_full, reduce_full, slope)
    dense_grad = scatter_row(mm(attended, cotangent_panel, TN), 1)
    reduce_grad = scatter_row(mm(activated, cotangent_panel, TN), 1)
    triple_back = attend_back(qkv, begin, attended_back, logsum, tables)
    both_part, row_sums, norm_grad = back(
        triple_back, query_full, hidden_back, expand_full, input_panel, stats, norm_params
    )
    both = lax.psum_scatter(both_part, "col", scatter_dimension=1, tiled=True)
    qkv_grad = scatter_row(mm(first_in, triple_back, TN), 0)
    expand_grad = scatter_row(mm(second_in, hidden_back, TN), 0)
    lanes = 128
    row_sums = total(row_sums.T.reshape(-1, lanes), ("col",)).reshape(2, row_count)
    norm_total = total(norm_grad.reshape(-1, lanes), ("col", "row")).reshape(4, features)
    output_sum = jnp.sum(grad_out, 0, dtype=jnp.float32)
    sums = jnp.concatenate(
        [jnp.sum(triple_back, 0, dtype=jnp.float32), output_sum, hidden_sum[0]]
    )
    sums = total(sums.reshape(-1, lanes), ("row",)).reshape(-1)
    query_bias_total = sums[: query_bias.shape[0]]
    output_total = sums[query_bias.shape[0] : query_bias.shape[0] + col_width]
    dense_total = jnp.stack([output_total, output_total])
    expand_total = sums[query_bias.shape[0] + col_width :]
    norm_slice = (tokens_in.astype(jnp.float32) - stats[:, 0:1]) * stats[:, 1:2]
    mean = (row_sums[0] / features)[:, None]
    cross = (row_sums[1] / features)[:, None]
    tokens_grad = grad_out.astype(jnp.float32) + stats[:, 1:2] * (
        both.astype(jnp.float32) - mean - norm_slice * cross
    )
    scaling = 1.0 / (row_count * lax.axis_size("row"))
    counter = step_count[0].astype(jnp.float32)
    new_qkv, new_query_left, new_query_right = shampoo(
        query_key_value,
        qkv_grad,
        query_left,
        query_right,
        query_left_root,
        query_right_root,
        scaling,
    )
    new_dense, new_attn_left, new_attn_right = shampoo(
        attn_dense, dense_grad, attn_left, attn_right, attn_left_root, attn_right_root, scaling
    )
    new_expand, new_expand_left, new_expand_right = shampoo(
        mlp_expand,
        expand_grad,
        expand_left,
        expand_right,
        expand_left_root,
        expand_right_root,
        scaling,
    )
    new_reduce, new_reduce_left, new_reduce_right = shampoo(
        mlp_reduce,
        reduce_grad,
        reduce_left,
        reduce_right,
        reduce_left_root,
        reduce_right_root,
        scaling,
    )
    new_norm, new_norm_one, new_norm_two = adam(
        norm_params, norm_first, norm_second, norm_total, scaling, counter
    )
    new_qbias, new_qbias_one, new_qbias_two = adam(
        query_bias, query_bias_first, query_bias_second, query_bias_total, scaling, counter
    )
    new_dbias, new_dbias_one, new_dbias_two = adam(
        dense_biases, dense_biases_first, dense_biases_second, dense_total, scaling, counter
    )
    new_ebias, new_ebias_one, new_ebias_two = adam(
        expand_bias, expand_bias_first, expand_bias_second, expand_total, scaling, counter
    )
    return (
        block_out,
        tokens_grad,
        qkv_grad,
        dense_grad,
        expand_grad,
        reduce_grad,
        new_qkv,
        new_dense,
        new_expand,
        new_reduce,
        new_query_left,
        new_query_right,
        new_attn_left,
        new_attn_right,
        new_expand_left,
        new_expand_right,
        new_reduce_left,
        new_reduce_right,
        new_norm,
        new_norm_one,
        new_norm_two,
        new_qbias,
        new_qbias_one,
        new_qbias_two,
        new_dbias,
        new_dbias_one,
        new_dbias_two,
        new_ebias,
        new_ebias_one,
        new_ebias_two,
    )


def solution(mesh):
    return jax.shard_map(
        local,
        mesh=mesh,
        in_specs=(
            P("row", "col"),
            P("row", "col"),
            P("row", None),
            P(),
            P("row", "col"),
            P("col", "row"),
            P("row", "col"),
            P("col", "row"),
            P(),
            P("col"),
            P(None, "col"),
            P("col"),
            P(),
            P(),
            P("col"),
            P("col"),
            P(None, "col"),
            P(None, "col"),
            P("col"),
            P("col"),
            P("row", "col", None, None),
            P("row", "col", None, None),
            P("col", "row", None, None),
            P("col", "row", None, None),
            P("row", "col", None, None),
            P("row", "col", None, None),
            P("col", "row", None, None),
            P("col", "row", None, None),
            P("row", "col", None, None),
            P("row", "col", None, None),
            P("col", "row", None, None),
            P("col", "row", None, None),
            P("row", "col", None, None),
            P("row", "col", None, None),
            P("col", "row", None, None),
            P("col", "row", None, None),
        ),
        out_specs=(
            P("row", "col"),
            P("row", "col"),
            P("row", "col"),
            P("col", "row"),
            P("row", "col"),
            P("col", "row"),
            P("row", "col"),
            P("col", "row"),
            P("row", "col"),
            P("col", "row"),
            P("row", "col", None, None),
            P("row", "col", None, None),
            P("col", "row", None, None),
            P("col", "row", None, None),
            P("row", "col", None, None),
            P("row", "col", None, None),
            P("col", "row", None, None),
            P("col", "row", None, None),
            P(),
            P(),
            P(),
            P("col"),
            P("col"),
            P("col"),
            P(None, "col"),
            P(None, "col"),
            P(None, "col"),
            P("col"),
            P("col"),
            P("col"),
        ),
        check_vma=False,
    )
```

```python
import functools
import math

import jax
import jax.numpy as jnp
from jax import lax
from jax.experimental import pallas as pl
from jax.experimental.pallas import tpu as pltpu
from jax.sharding import Mesh, PartitionSpec as P


COL = ("far", "near")
HD = 128
ROT = 32


NORM_EPS = 1e-05
ROPE_BASE = 10000.0
MASKED = -1e30
SHAMPOO_DECAY = 0.95
MATRIX_RATE = 0.5
WEIGHT_DECAY = 0.01
FIRST_DECAY = 0.9
SECOND_DECAY = 0.95
VECTOR_RATE = 0.6
ADAM_EPS = 1e-08

NT = (((1,), (1,)), ((), ()))
TN = (((0,), (0,)), ((), ()))
NN = (((1,), (0,)), ((), ()))
VMEM_BYTES = 60 * 1024 * 1024


def mm(a, b, dims=NN):
    return lax.dot_general(a, b, dims, preferred_element_type=jnp.float32)


def params(*semantics):
    return pltpu.CompilerParams(dimension_semantics=semantics, vmem_limit_bytes=VMEM_BYTES)


def cost(flops, moved, exps=0):
    return pl.CostEstimate(flops=int(flops), bytes_accessed=int(moved), transcendentals=int(exps))


def whole(shape):
    return pl.BlockSpec(
        shape, lambda *_: (0,) * len(shape), pipeline_mode=pl.Buffered(buffer_count=1)
    )


def halves(tile, width, blocks):
    half = blocks // 2
    return [
        pl.BlockSpec((tile, width), lambda i, _: (jnp.minimum(i, half - 1), 0)),
        pl.BlockSpec((tile, width), lambda i, _: (jnp.maximum(i - half, 0), 0)),
    ]


def assemble(near, width, mine, other, panel_ref):
    half = pl.num_programs(0) // 2
    for number in range(2):

        @pl.when((pl.program_id(0) >= half) == bool(number))
        def _():
            for far in range(panel_ref.shape[1] // (2 * width)):
                at = slice(far * width, (far + 1) * width)
                here = pl.multiple_of((2 * far + near) * width, width)
                there = pl.multiple_of((2 * far + 1 - near) * width, width)
                panel_ref[:, pl.ds(here, width)] = mine[number][:, at]
                panel_ref[:, pl.ds(there, width)] = other[number][:, at]


def positions(lengths, number):
    tokens = jnp.arange(number, dtype=jnp.int32)
    endings = jnp.cumsum(lengths, dtype=jnp.int32)
    finished = (endings[None, :] <= tokens[:, None]).astype(jnp.int32)
    return jnp.sum(finished * lengths[None, :], -1, dtype=jnp.int32)


def rotary_tables(places):
    middle = ROT // 2
    indices = jnp.arange(middle, dtype=jnp.float32)
    inverse = jnp.exp(indices * (-2.0 * math.log(ROPE_BASE) / ROT))
    angles = places.astype(jnp.float32)[:, None] * inverse[None, :]
    cosine, sine = jnp.cos(angles), jnp.sin(angles)
    number = places.shape[0]
    ones = jnp.ones((number, HD - ROT), jnp.float32)
    gap = jnp.zeros((number, middle), jnp.float32)
    rest = jnp.zeros((number, HD - ROT), jnp.float32)
    return (
        jnp.concatenate([cosine, cosine, ones], -1),
        jnp.concatenate([-sine, gap, rest], -1),
        jnp.concatenate([gap, sine, rest], -1),
    )


def turn(vectors, own, ahead, behind):
    middle = ROT // 2
    return (
        vectors * own
        + pltpu.roll(vectors, HD - middle, 1) * ahead
        + pltpu.roll(vectors, middle, 1) * behind
    )


def front_kernel(
    share, near_ref, mine_first, mine_second, other_first, other_second,
    norm_ref, wq_ref, qb_ref, own_ref, ahead_ref, behind_ref, we_ref, eb_ref,
    x_ref, one_ref, two_ref, stat_ref, qkv_ref, act_ref, slope_ref,
):
    assemble(
        near_ref[0], share, (mine_first, mine_second), (other_first, other_second), x_ref
    )
    x = x_ref[...].astype(jnp.float32)
    mu = jnp.mean(x, -1, keepdims=True)
    center = x - mu
    inverse = lax.rsqrt(jnp.mean(center * center, -1, keepdims=True) + NORM_EPS)
    normalized = center * inverse
    stat_ref[...] = jnp.concatenate([mu, inverse], -1)
    one = (normalized * norm_ref[0:1] + norm_ref[1:2]).astype(jnp.bfloat16)
    two = (normalized * norm_ref[2:3] + norm_ref[3:4]).astype(jnp.bfloat16)
    one_ref[...] = one
    two_ref[...] = two
    own, ahead, behind = own_ref[...], ahead_ref[...], behind_ref[...]
    for head in range(wq_ref.shape[1] // (3 * HD)):
        cols = slice(head * 3 * HD, (head + 1) * 3 * HD)
        triple = mm(one, wq_ref[:, cols]) + qb_ref[:, cols]
        query = turn(triple[:, :HD], own, ahead, behind)
        key = turn(triple[:, HD : 2 * HD], own, ahead, behind)
        qkv_ref[:, cols] = jnp.concatenate([query, key, triple[:, 2 * HD :]], -1).astype(
            jnp.bfloat16
        )
    width = 256
    for first in range(0, we_ref.shape[1], width):
        cols = slice(first, first + width)
        hidden = mm(two, we_ref[:, cols]) + eb_ref[:, cols]
        phi = 0.5 + 0.5 * lax.erf(hidden * (0.5**0.5))
        act_ref[:, cols] = (hidden * phi).astype(jnp.bfloat16)
        density = jnp.exp(-0.5 * hidden * hidden) * ((0.5 / math.pi) ** 0.5)
        slope_ref[:, cols] = phi + hidden * density


def front(near, share, mine, other, norm_params, wq, qbias, tables, we, ebias):
    tokens, features = 2 * mine[0].shape[0], 2 * mine[0].shape[1]
    tile = 256
    blocks = tokens // tile
    wide, hidden = wq.shape[1], we.shape[1]

    def rows(width):
        return pl.BlockSpec((tile, width), lambda i, _: (i, 0))

    return pl.pallas_call(
        functools.partial(front_kernel, share),
        grid_spec=pltpu.PrefetchScalarGridSpec(
            num_scalar_prefetch=1,
            grid=(blocks,),
        in_specs=[
            *halves(tile, features // 2, blocks),
            *halves(tile, features // 2, blocks),
            whole(norm_params.shape),
            whole(wq.shape),
            whole((1, wide)),
            rows(HD),
            rows(HD),
            rows(HD),
            whole(we.shape),
            whole((1, hidden)),
        ],
        out_specs=[
            rows(features),
            rows(features),
            rows(features),
            rows(2),
            rows(wide),
            rows(hidden),
            rows(hidden),
        ],
        ),
        out_shape=[
            jax.ShapeDtypeStruct((tokens, features), jnp.bfloat16),
            jax.ShapeDtypeStruct((tokens, features), jnp.bfloat16),
            jax.ShapeDtypeStruct((tokens, features), jnp.bfloat16),
            jax.ShapeDtypeStruct((tokens, 2), jnp.float32),
            jax.ShapeDtypeStruct((tokens, wide), jnp.bfloat16),
            jax.ShapeDtypeStruct((tokens, hidden), jnp.bfloat16),
            jax.ShapeDtypeStruct((tokens, hidden), jnp.float32),
        ],
        compiler_params=params("arbitrary"),
        cost_estimate=cost(
            2 * tokens * features * (wide + hidden), tokens * (6 * features + 2 * wide + 6 * hidden)
        ),
        name="front",
    )(near, *mine, *other, norm_params, wq, qbias[None], *tables, we, ebias[None])


def scores(q, k, rows, begin, start):
    raw = mm(q, k, NT) * HD**-0.5
    cols = start + lax.broadcasted_iota(jnp.int32, raw.shape, 1)
    return raw, (cols >= begin) & (cols <= rows)


def attend_kernel(from_ref, q_ref, k_ref, v_ref, begin_ref, out_ref, sum_ref, held):
    tile, span = q_ref.shape[0], held.shape[2]
    block = pl.program_id(1)
    low, high = from_ref[block], (block * tile + tile - 1) // span + 1
    q, begin = q_ref[...], begin_ref[...]
    rows = block * tile + lax.broadcasted_iota(jnp.int32, (tile, 1), 0)

    def first_pass(j, top):
        start = pl.multiple_of(j * span, span)
        raw, allowed = scores(q, k_ref[pl.ds(start, span)], rows, begin, start)
        raw = jnp.where(allowed, raw, MASKED)
        held[j] = raw
        return jnp.maximum(top, jnp.max(raw, -1, keepdims=True))

    top = lax.fori_loop(low, high, first_pass, jnp.full((tile, 1), MASKED, jnp.float32))

    def second_pass(j, carry):
        total, out = carry
        start = pl.multiple_of(j * span, span)
        weights = jnp.exp(held[j] - top)
        total = total + jnp.sum(weights, -1, keepdims=True)
        return total, out + mm(weights.astype(jnp.bfloat16), v_ref[pl.ds(start, span)])

    total, out = lax.fori_loop(
        low,
        high,
        second_pass,
        (jnp.zeros((tile, 1), jnp.float32), jnp.zeros((tile, HD), jnp.float32)),
    )
    out_ref[...] = (out / total).astype(jnp.bfloat16)
    sum_ref[...] = top + jnp.log(total)


def tiles(length):
    return min(256, length), min(512, length)


def attend(qkv, begin):
    length = qkv.shape[0]
    heads = qkv.shape[1] // (3 * HD)
    tile, span = tiles(length)
    grid_spec = pltpu.PrefetchScalarGridSpec(
        num_scalar_prefetch=1,
        grid=(heads, length // tile),
        in_specs=[
            pl.BlockSpec((tile, HD), lambda h, i, _: (i, 3 * h)),
            pl.BlockSpec((length, HD), lambda h, i, _: (0, 3 * h + 1)),
            pl.BlockSpec((length, HD), lambda h, i, _: (0, 3 * h + 2)),
            pl.BlockSpec((tile, 1), lambda h, i, _: (i, 0)),
        ],
        out_specs=[
            pl.BlockSpec((tile, HD), lambda h, i, _: (i, h)),
            pl.BlockSpec((None, tile, 1), lambda h, i, _: (h, i, 0)),
        ],
        scratch_shapes=[pltpu.VMEM((length // span, tile, span), jnp.float32)],
    )
    return pl.pallas_call(
        attend_kernel,
        grid_spec=grid_spec,
        out_shape=[
            jax.ShapeDtypeStruct((length, heads * HD), jnp.bfloat16),
            jax.ShapeDtypeStruct((heads, length, 1), jnp.float32),
        ],
        compiler_params=params("arbitrary", "arbitrary"),
        cost_estimate=cost(4 * heads * length * length * HD, 8 * heads * length * HD, heads * length * length),
        name="attend",
    )(begin[::tile] // span, qkv, qkv, qkv, begin[:, None])


def attend_back_kernel(
    from_ref, q_ref, k_ref, v_ref, grad_ref, begin_ref, sum_ref, own_ref, ahead_ref, behind_ref,
    out_ref, probs, probs_back, key_back, value_back,
):
    tile, span = q_ref.shape[0], probs.shape[2]
    block, blocks = pl.program_id(1), pl.num_programs(1)
    low, high = from_ref[block], (block * tile + tile - 1) // span + 1
    q, grad, begin, logsum = q_ref[...], grad_ref[...], begin_ref[...], sum_ref[...]
    rows = block * tile + lax.broadcasted_iota(jnp.int32, (tile, 1), 0)

    @pl.when(block == 0)
    def _():
        key_back[...] = jnp.zeros_like(key_back)
        value_back[...] = jnp.zeros_like(value_back)

    def first_pass(j, inner):
        start = pl.multiple_of(j * span, span)
        raw, allowed = scores(q, k_ref[pl.ds(start, span)], rows, begin, start)
        weights = jnp.where(allowed, jnp.exp(raw - logsum), 0.0)
        back = mm(grad, v_ref[pl.ds(start, span)], NT)
        probs[j] = weights
        probs_back[j] = back
        return inner + jnp.sum(weights * back, -1, keepdims=True)

    inner = lax.fori_loop(low, high, first_pass, jnp.zeros((tile, 1), jnp.float32))

    def second_pass(j, query_back):
        start = pl.multiple_of(j * span, span)
        weights = probs[j]
        raw_back = (weights * (probs_back[j] - inner) * HD**-0.5).astype(jnp.bfloat16)
        part = pl.ds(start, span)
        key_back[part] += mm(raw_back, q, TN)
        value_back[part] += mm(weights.astype(jnp.bfloat16), grad, TN)
        return query_back + mm(raw_back, k_ref[part])

    query_back = lax.fori_loop(low, high, second_pass, jnp.zeros((tile, HD), jnp.float32))
    here = pl.ds(pl.multiple_of(block * tile, tile), tile)
    query_back = turn(query_back, own_ref[here], -ahead_ref[here], -behind_ref[here])
    out_ref[here, :HD] = query_back.astype(jnp.bfloat16)

    @pl.when(block == blocks - 1)
    def _():
        def finish(i, _):
            at = pl.ds(pl.multiple_of(i * tile, tile), tile)
            keys = turn(key_back[at], own_ref[at], -ahead_ref[at], -behind_ref[at])
            out_ref[at, HD : 2 * HD] = keys.astype(jnp.bfloat16)
            out_ref[at, 2 * HD :] = value_back[at].astype(jnp.bfloat16)
            return 0

        lax.fori_loop(0, blocks, finish, 0)


def attend_back(qkv, begin, grad, logsum, tables):
    length = qkv.shape[0]
    heads = qkv.shape[1] // (3 * HD)
    tile, span = tiles(length)
    grid_spec = pltpu.PrefetchScalarGridSpec(
        num_scalar_prefetch=1,
        grid=(heads, length // tile),
        in_specs=[
            pl.BlockSpec((tile, HD), lambda h, i, _: (i, 3 * h)),
            pl.BlockSpec((length, HD), lambda h, i, _: (0, 3 * h + 1)),
            pl.BlockSpec((length, HD), lambda h, i, _: (0, 3 * h + 2)),
            pl.BlockSpec((tile, HD), lambda h, i, _: (i, h)),
            pl.BlockSpec((tile, 1), lambda h, i, _: (i, 0)),
            pl.BlockSpec((None, tile, 1), lambda h, i, _: (h, i, 0)),
            whole((length, HD)),
            whole((length, HD)),
            whole((length, HD)),
        ],
        out_specs=[pl.BlockSpec((length, 3 * HD), lambda h, i, _: (0, h))],
        scratch_shapes=[
            pltpu.VMEM((length // span, tile, span), jnp.float32),
            pltpu.VMEM((length // span, tile, span), jnp.float32),
            pltpu.VMEM((length, HD), jnp.float32),
            pltpu.VMEM((length, HD), jnp.float32),
        ],
    )
    return pl.pallas_call(
        attend_back_kernel,
        grid_spec=grid_spec,
        out_shape=[jax.ShapeDtypeStruct(qkv.shape, jnp.bfloat16)],
        compiler_params=params("arbitrary", "arbitrary"),
        cost_estimate=cost(10 * heads * length * length * HD, 14 * heads * length * HD, heads * length * length),
        name="attend_back",
    )(begin[::tile] // span, qkv, qkv, qkv, grad, begin[:, None], logsum, *tables)[0]


def join_kernel(
    share, near_ref, a_ref, wa_ref, b_ref, wb_ref,
    keep_first, keep_second, away_first, away_second,
):
    near = near_ref[0]
    a, b = a_ref[...], b_ref[...]
    half = pl.num_programs(0) // 2
    for number, keep_ref, away_ref in (
        (0, keep_first, away_first),
        (1, keep_second, away_second),
    ):

        @pl.when((pl.program_id(0) >= half) == bool(number))
        def _():
            def far(f, _):
                at = pl.ds(pl.multiple_of(f * share, share), share)
                here = pl.ds(pl.multiple_of((2 * f + near) * share, share), share)
                there = pl.ds(pl.multiple_of((2 * f + 1 - near) * share, share), share)
                keep_ref[:, at] = mm(a, wa_ref[:, here]) + mm(b, wb_ref[:, here])
                away = mm(a, wa_ref[:, there]) + mm(b, wb_ref[:, there])
                away_ref[:, at] = away.astype(jnp.bfloat16)
                return 0

            lax.fori_loop(0, keep_ref.shape[1] // share, far, 0, unroll=True)


def join(near, share, a, wa, b, wb):
    tokens, features = a.shape[0], wa.shape[1]
    tile = 256
    blocks = tokens // tile
    half = (tokens // 2, features // 2)
    return pl.pallas_call(
        functools.partial(join_kernel, share),
        grid_spec=pltpu.PrefetchScalarGridSpec(
            num_scalar_prefetch=1,
            grid=(blocks,),
            in_specs=[
                pl.BlockSpec((tile, a.shape[1]), lambda i, _: (i, 0)),
                whole(wa.shape),
                pl.BlockSpec((tile, b.shape[1]), lambda i, _: (i, 0)),
                whole(wb.shape),
            ],
            out_specs=[
                *halves(tile, features // 2, blocks),
                *halves(tile, features // 2, blocks),
            ],
        ),
        out_shape=[
            jax.ShapeDtypeStruct(half, jnp.float32),
            jax.ShapeDtypeStruct(half, jnp.float32),
            jax.ShapeDtypeStruct(half, jnp.bfloat16),
            jax.ShapeDtypeStruct(half, jnp.bfloat16),
        ],
        compiler_params=params("arbitrary"),
        cost_estimate=cost(2 * tokens * features * (a.shape[1] + b.shape[1]), 6 * tokens * features),
        name="join",
    )(near, a, wa, b, wb)


def part_kernel(
    share, near_ref, mine_first, mine_second, other_first, other_second,
    wd_ref, wr_ref, slope_ref, g_ref, att_ref, hid_ref, sum_ref,
):
    assemble(
        near_ref[0], share, (mine_first, mine_second), (other_first, other_second), g_ref
    )
    g = g_ref[...]
    att_ref[...] = mm(g, wd_ref[...], NT).astype(jnp.bfloat16)

    @pl.when(pl.program_id(0) == 0)
    def _():
        sum_ref[...] = jnp.zeros_like(sum_ref)

    width = 256
    for first in range(0, wr_ref.shape[0], width):
        cols = slice(first, first + width)
        back = (mm(g, wr_ref[cols], NT) * slope_ref[:, cols]).astype(jnp.bfloat16)
        hid_ref[:, cols] = back
        sum_ref[:, cols] += jnp.sum(back.astype(jnp.float32), 0, keepdims=True)


def part(near, share, mine, other, wd, wr, slope):
    tokens, features = 2 * mine[0].shape[0], 2 * mine[0].shape[1]
    tile = 256
    blocks = tokens // tile

    def rows(width):
        return pl.BlockSpec((tile, width), lambda i, _: (i, 0))

    return pl.pallas_call(
        functools.partial(part_kernel, share),
        grid_spec=pltpu.PrefetchScalarGridSpec(
            num_scalar_prefetch=1,
            grid=(blocks,),
        in_specs=[
            *halves(tile, features // 2, blocks),
            *halves(tile, features // 2, blocks),
            whole(wd.shape),
            whole(wr.shape),
            rows(wr.shape[0]),
        ],
        out_specs=[
            rows(features),
            rows(wd.shape[0]),
            rows(wr.shape[0]),
            pl.BlockSpec((1, wr.shape[0]), lambda i, _: (0, 0)),
        ],
        ),
        out_shape=[
            jax.ShapeDtypeStruct((tokens, features), jnp.bfloat16),
            jax.ShapeDtypeStruct((tokens, wd.shape[0]), jnp.bfloat16),
            jax.ShapeDtypeStruct((tokens, wr.shape[0]), jnp.bfloat16),
            jax.ShapeDtypeStruct((1, wr.shape[0]), jnp.float32),
        ],
        compiler_params=params("arbitrary"),
        cost_estimate=cost(
            2 * tokens * features * (wd.shape[0] + wr.shape[0]), tokens * (2 * features + 8 * wr.shape[0])
        ),
        name="part",
    )(near, *mine, *other, wd, wr, slope)


def back_kernel(
    share, near_ref, tb_ref, wq_ref, hb_ref, we_ref, x_ref, stat_ref, norm_ref,
    keep_first, keep_second, away_first, away_second, row_ref, col_ref,
):
    near = near_ref[0]
    half = pl.num_programs(0) // 2

    @pl.when(pl.program_id(0) == 0)
    def _():
        col_ref[...] = jnp.zeros_like(col_ref)

    triple_back, hidden_back = tb_ref[...], hb_ref[...]
    mu, inverse = stat_ref[:, 0:1], stat_ref[:, 1:2]

    def block(number, plain, crossed):
        cols = pl.ds(pl.multiple_of(number * share, share), share)
        one = mm(triple_back, wq_ref[cols], NT)
        two = mm(hidden_back, we_ref[cols], NT)
        normalized = (x_ref[:, cols].astype(jnp.float32) - mu) * inverse
        col_ref[:, cols] += jnp.concatenate(
            [
                jnp.sum(one * normalized, 0, keepdims=True),
                jnp.sum(one, 0, keepdims=True),
                jnp.sum(two * normalized, 0, keepdims=True),
                jnp.sum(two, 0, keepdims=True),
            ],
            0,
        )
        both = one * norm_ref[0:1, cols] + two * norm_ref[2:3, cols]
        plain = plain + jnp.sum(both, -1, keepdims=True)
        return both, plain, crossed + jnp.sum(both * normalized, -1, keepdims=True)

    zero = jnp.zeros((tb_ref.shape[0], 1), jnp.float32)
    for number, keep_ref, away_ref in (
        (0, keep_first, away_first),
        (1, keep_second, away_second),
    ):

        @pl.when((pl.program_id(0) >= half) == bool(number))
        def _():
            def far(f, carry):
                at = pl.ds(pl.multiple_of(f * share, share), share)
                both, plain, crossed = block(2 * f + near, *carry)
                keep_ref[:, at] = both
                both, plain, crossed = block(2 * f + 1 - near, plain, crossed)
                away_ref[:, at] = both.astype(jnp.bfloat16)
                return plain, crossed

            plain, crossed = lax.fori_loop(
                0, keep_ref.shape[1] // share, far, (zero, zero), unroll=True
            )
            row_ref[...] = jnp.concatenate([plain, crossed], -1)


def back(near, share, triple_back, wq, hidden_back, we, panel, stats, norm_params):
    tokens, features = panel.shape
    tile = 256
    blocks = tokens // tile
    half = (tokens // 2, features // 2)

    def rows(width):
        return pl.BlockSpec((tile, width), lambda i, _: (i, 0))

    return pl.pallas_call(
        functools.partial(back_kernel, share),
        grid_spec=pltpu.PrefetchScalarGridSpec(
            num_scalar_prefetch=1,
            grid=(blocks,),
            in_specs=[
                rows(wq.shape[1]),
                whole(wq.shape),
                rows(we.shape[1]),
                whole(we.shape),
                rows(features),
                rows(2),
                whole(norm_params.shape),
            ],
            out_specs=[
                *halves(tile, features // 2, blocks),
                *halves(tile, features // 2, blocks),
                rows(2),
                pl.BlockSpec((4, features), lambda i, _: (0, 0)),
            ],
        ),
        out_shape=[
            jax.ShapeDtypeStruct(half, jnp.float32),
            jax.ShapeDtypeStruct(half, jnp.float32),
            jax.ShapeDtypeStruct(half, jnp.bfloat16),
            jax.ShapeDtypeStruct(half, jnp.bfloat16),
            jax.ShapeDtypeStruct((tokens, 2), jnp.float32),
            jax.ShapeDtypeStruct((4, features), jnp.float32),
        ],
        compiler_params=params("arbitrary"),
        cost_estimate=cost(
            2 * tokens * features * (wq.shape[1] + we.shape[1]), tokens * 8 * features
        ),
        name="back",
    )(near, triple_back, wq, hidden_back, we, panel, stats, norm_params)


def shampoo_kernel(scaling, w_ref, g_ref, l_ref, r_ref, p_ref, q_ref, nw_ref, nl_ref, nr_ref):
    size = l_ref.shape[-1]
    for block in range(l_ref.shape[1]):
        cols = slice(block * size, (block + 1) * size)
        grad = (g_ref[:, cols] * scaling).astype(jnp.bfloat16)
        nl_ref[0, block] = SHAMPOO_DECAY * l_ref[0, block] + (1.0 - SHAMPOO_DECAY) * mm(grad, grad, NT)
        nr_ref[0, block] = SHAMPOO_DECAY * r_ref[0, block] + (1.0 - SHAMPOO_DECAY) * mm(grad, grad, TN)
        turned = mm(p_ref[0, block].astype(jnp.bfloat16), grad).astype(jnp.bfloat16)
        step = mm(turned, q_ref[0, block].astype(jnp.bfloat16))
        weight = w_ref[:, cols]
        nw_ref[:, cols] = weight - MATRIX_RATE * (step + WEIGHT_DECAY * weight)


def shampoo(weight, gradient, left_stat, right_stat, left_root, right_root, scaling):
    height, breadth = gradient.shape
    size = left_stat.shape[-1]
    across = breadth // size
    flat = pl.BlockSpec((size, breadth), lambda i: (i, 0))
    cube = pl.BlockSpec((1, across, size, size), lambda i: (i, 0, 0, 0))
    return pl.pallas_call(
        functools.partial(shampoo_kernel, scaling),
        grid=(height // size,),
        in_specs=[flat, flat, cube, cube, cube, cube],
        out_specs=[flat, cube, cube],
        out_shape=[
            jax.ShapeDtypeStruct(weight.shape, jnp.float32),
            jax.ShapeDtypeStruct(left_stat.shape, jnp.float32),
            jax.ShapeDtypeStruct(right_stat.shape, jnp.float32),
        ],
        compiler_params=params("arbitrary"),
        cost_estimate=cost(8 * height * breadth * size, 36 * height * breadth),
    )(weight, gradient, left_stat, right_stat, left_root, right_root)


def swap(value, axis, bit):
    size = lax.axis_size(axis)
    return lax.ppermute(value, axis, [(i, i ^ bit) for i in range(size)])


def gather_row(shard, dim):
    if lax.axis_size("row") != 4:
        return lax.all_gather(shard, "row", axis=dim, tiled=True)
    me = lax.axis_index("row")
    across = swap(shard, "row", 2)
    beside = swap(shard, "row", 1)
    corner = swap(across, "row", 1)
    shape = list(shard.shape)
    step = shape[dim]
    shape[dim] *= 4
    out = jnp.zeros(shape, shard.dtype)
    for bit, piece in ((0, shard), (2, across), (1, beside), (3, corner)):
        out = lax.dynamic_update_slice_in_dim(out, piece, (me ^ bit) * step, dim)
    return out


def scatter_row(value, dim):
    if lax.axis_size("row") != 4:
        return lax.psum_scatter(value, "row", scatter_dimension=dim, tiled=True)
    me = lax.axis_index("row")
    step = value.shape[dim] // 4

    def share(owner):
        return lax.dynamic_slice_in_dim(value, owner * step, step, dim)

    far_beside = swap(share(me ^ 3).astype(jnp.bfloat16), "row", 1)
    near_beside = swap(share(me ^ 1).astype(jnp.bfloat16), "row", 1)
    far = share(me ^ 2) + far_beside.astype(jnp.float32)
    across = swap(far.astype(jnp.bfloat16), "row", 2)
    return share(me) + near_beside.astype(jnp.float32) + across.astype(jnp.float32)


def total(value, axes):
    for axis in axes:
        bit = 1
        while bit < lax.axis_size(axis):
            value = value + swap(value, axis, bit)
            bit *= 2
    return value


def gather_far(value):
    half = value.shape[0] // 2
    return [
        lax.all_gather(value[first : first + half], "far", axis=1, tiled=True)
        for first in (0, half)
    ]


def scatter_far(both):
    return lax.psum_scatter(both, "far", scatter_dimension=1, tiled=True)


def pair_sum(kept, received):
    return (kept + received.astype(jnp.float32)).astype(jnp.bfloat16)


def product(a, b):
    return mm(a, b, TN)


def after(value, *others):
    return lax.optimization_barrier((value, *others))[0]


def adam(vector, moment_one, moment_two, gradient, scaling, counter):
    mean_grad = gradient * scaling
    new_one = FIRST_DECAY * moment_one + (1.0 - FIRST_DECAY) * mean_grad
    new_two = SECOND_DECAY * moment_two + (1.0 - SECOND_DECAY) * mean_grad * mean_grad
    first_hat = new_one / (1.0 - FIRST_DECAY**counter)
    second_hat = new_two / (1.0 - SECOND_DECAY**counter)
    new_vector = vector - VECTOR_RATE * first_hat / (jnp.sqrt(second_hat) + ADAM_EPS)
    return (new_vector, new_one, new_two)


def local(
    tokens_in,
    grad_out,
    sequence_lengths,
    step_count,
    query_key_value,
    attn_dense,
    mlp_expand,
    mlp_reduce,
    norm_params,
    query_bias,
    dense_biases,
    expand_bias,
    norm_first,
    norm_second,
    query_bias_first,
    query_bias_second,
    dense_biases_first,
    dense_biases_second,
    expand_bias_first,
    expand_bias_second,
    query_left,
    query_right,
    attn_left,
    attn_right,
    expand_left,
    expand_right,
    reduce_left,
    reduce_right,
    query_left_root,
    query_right_root,
    attn_left_root,
    attn_right_root,
    expand_left_root,
    expand_right_root,
    reduce_left_root,
    reduce_right_root,
):
    input_mine, cotangent_mine = gather_far(tokens_in), gather_far(grad_out)
    input_other = [swap(piece, "near", 1) for piece in input_mine]
    query_full = gather_row(query_key_value.astype(jnp.bfloat16), 0)
    expand_full = gather_row(mlp_expand.astype(jnp.bfloat16), 0)
    dense_full = gather_row(attn_dense.astype(jnp.bfloat16), 1)
    reduce_full = gather_row(mlp_reduce.astype(jnp.bfloat16), 1)
    row_count, col_width = tokens_in.shape
    features = norm_params.shape[1]
    near = lax.axis_index("near").astype(jnp.int32)[None]
    begin = positions(sequence_lengths[0], row_count)
    tables = rotary_tables(jnp.arange(row_count, dtype=jnp.int32) - begin)
    input_panel, first_in, second_in, stats, qkv, activated, slope = front(
        near, col_width, input_mine, input_other, norm_params,
        query_full, query_bias, tables, expand_full, expand_bias,
    )
    cotangent_other = [
        swap(cotangent_mine[0], "near", 1), swap(after(cotangent_mine[1], stats), "near", 1)
    ]
    attended, logsum = attend(qkv, begin)
    *branches_kept, sent_first, sent_second = join(
        near, col_width, attended, dense_full, activated, reduce_full
    )
    branches_got = [swap(sent_first, "near", 1), swap(sent_second, "near", 1)]
    output_sum = jnp.sum(after(grad_out, sent_first), 0, dtype=jnp.float32)
    cotangent_panel, attended_back, hidden_back, hidden_sum = part(
        near, col_width, cotangent_mine, cotangent_other, dense_full, reduce_full,
        after(slope, sent_first),
    )
    triple_back = attend_back(qkv, begin, attended_back, logsum, tables)
    branch_sum = pair_sum(branches_kept[0], after(branches_got[0], triple_back))
    branch_first = scatter_far(branch_sum)
    *both_kept, sent_first, sent_second, row_sums, norm_grad = back(
        near, col_width, after(triple_back, branch_sum), query_full, hidden_back, expand_full,
        input_panel, stats, norm_params,
    )
    both_got = [swap(sent_first, "near", 1), swap(sent_second, "near", 1)]
    cotangent_late = after(cotangent_panel, sent_first)
    reduce_part = product(activated, cotangent_late)
    reduce_grad = scatter_row(reduce_part, 1)
    dense_part = product(attended, cotangent_late)
    dense_grad = scatter_row(dense_part, 1)
    branch_sum = pair_sum(branches_kept[1], after(branches_got[1], dense_part, reduce_part))
    branch_second = scatter_far(branch_sum)
    expand_part = product(after(second_in, branch_sum), hidden_back)
    expand_grad = scatter_row(expand_part, 0)
    qkv_part = product(after(first_in, branch_sum), triple_back)
    qkv_grad = scatter_row(qkv_part, 0)
    first_sum = pair_sum(both_kept[0], after(both_got[0], qkv_part, expand_part))
    both_first = scatter_far(first_sum)
    lanes = 128
    row_sums = total(row_sums.T.reshape(-1, lanes), ("near", "far")).reshape(2, row_count)
    norm_total = total(norm_grad.reshape(-1, lanes), ("near", "far", "row")).reshape(4, features)
    sums = jnp.concatenate(
        [jnp.sum(triple_back, 0, dtype=jnp.float32), output_sum, hidden_sum[0]]
    )
    sums = total(sums.reshape(-1, lanes), ("row",)).reshape(-1)
    query_bias_total = sums[: query_bias.shape[0]]
    output_total = sums[query_bias.shape[0] : query_bias.shape[0] + col_width]
    dense_total = jnp.stack([output_total, output_total])
    expand_total = sums[query_bias.shape[0] + col_width :]
    norm_slice = (tokens_in.astype(jnp.float32) - stats[:, 0:1]) * stats[:, 1:2]
    scaling = 1.0 / (row_count * lax.axis_size("row"))
    counter = step_count[0].astype(jnp.float32)
    new_dense, new_attn_left, new_attn_right = shampoo(
        attn_dense,
        after(dense_grad, qkv_part, expand_part),
        attn_left,
        attn_right,
        attn_left_root,
        attn_right_root,
        scaling,
    )
    new_reduce, new_reduce_left, new_reduce_right = shampoo(
        mlp_reduce,
        after(reduce_grad, qkv_part, expand_part),
        reduce_left,
        reduce_right,
        reduce_left_root,
        reduce_right_root,
        scaling,
    )
    second_sum = pair_sum(both_kept[1], after(both_got[1], new_dense, new_reduce))
    both_second = scatter_far(second_sum)
    new_qkv, new_query_left, new_query_right = shampoo(
        query_key_value,
        after(qkv_grad, second_sum),
        query_left,
        query_right,
        query_left_root,
        query_right_root,
        scaling,
    )
    new_expand, new_expand_left, new_expand_right = shampoo(
        mlp_expand,
        after(expand_grad, second_sum),
        expand_left,
        expand_right,
        expand_left_root,
        expand_right_root,
        scaling,
    )
    branch_share, both = (
        jnp.concatenate([first, after(second, new_qkv, new_expand)], 0).astype(jnp.float32)
        for first, second in ((branch_first, branch_second), (both_first, both_second))
    )
    block_out = tokens_in.astype(jnp.float32) + branch_share + dense_biases[0] + dense_biases[1]
    mean = (row_sums[0] / features)[:, None]
    cross = (row_sums[1] / features)[:, None]
    tokens_grad = grad_out.astype(jnp.float32) + stats[:, 1:2] * (
        both - mean - norm_slice * cross
    )
    new_norm, new_norm_one, new_norm_two = adam(
        norm_params, norm_first, norm_second, norm_total, scaling, counter
    )
    new_qbias, new_qbias_one, new_qbias_two = adam(
        query_bias, query_bias_first, query_bias_second, query_bias_total, scaling, counter
    )
    new_dbias, new_dbias_one, new_dbias_two = adam(
        dense_biases, dense_biases_first, dense_biases_second, dense_total, scaling, counter
    )
    new_ebias, new_ebias_one, new_ebias_two = adam(
        expand_bias, expand_bias_first, expand_bias_second, expand_total, scaling, counter
    )
    return (
        block_out,
        tokens_grad,
        qkv_grad,
        dense_grad,
        expand_grad,
        reduce_grad,
        new_qkv,
        new_dense,
        new_expand,
        new_reduce,
        new_query_left,
        new_query_right,
        new_attn_left,
        new_attn_right,
        new_expand_left,
        new_expand_right,
        new_reduce_left,
        new_reduce_right,
        new_norm,
        new_norm_one,
        new_norm_two,
        new_qbias,
        new_qbias_one,
        new_qbias_two,
        new_dbias,
        new_dbias_one,
        new_dbias_two,
        new_ebias,
        new_ebias_one,
        new_ebias_two,
    )


def solution(mesh):
    rows, cols = mesh.shape["row"], mesh.shape["col"]
    split = Mesh(mesh.devices.reshape(rows, cols // 2, 2), ("row", *COL))
    return jax.shard_map(
        local,
        mesh=split,
        in_specs=(
            P("row", COL),
            P("row", COL),
            P("row", None),
            P(),
            P("row", COL),
            P(COL, "row"),
            P("row", COL),
            P(COL, "row"),
            P(),
            P(COL),
            P(None, COL),
            P(COL),
            P(),
            P(),
            P(COL),
            P(COL),
            P(None, COL),
            P(None, COL),
            P(COL),
            P(COL),
            P("row", COL, None, None),
            P("row", COL, None, None),
            P(COL, "row", None, None),
            P(COL, "row", None, None),
            P("row", COL, None, None),
            P("row", COL, None, None),
            P(COL, "row", None, None),
            P(COL, "row", None, None),
            P("row", COL, None, None),
            P("row", COL, None, None),
            P(COL, "row", None, None),
            P(COL, "row", None, None),
            P("row", COL, None, None),
            P("row", COL, None, None),
            P(COL, "row", None, None),
            P(COL, "row", None, None),
        ),
        out_specs=(
            P("row", COL),
            P("row", COL),
            P("row", COL),
            P(COL, "row"),
            P("row", COL),
            P(COL, "row"),
            P("row", COL),
            P(COL, "row"),
            P("row", COL),
            P(COL, "row"),
            P("row", COL, None, None),
            P("row", COL, None, None),
            P(COL, "row", None, None),
            P(COL, "row", None, None),
            P("row", COL, None, None),
            P("row", COL, None, None),
            P(COL, "row", None, None),
            P(COL, "row", None, None),
            P(),
            P(),
            P(),
            P(COL),
            P(COL),
            P(COL),
            P(None, COL),
            P(None, COL),
            P(None, COL),
            P(COL),
            P(COL),
            P(COL),
        ),
        check_vma=False,
    )
```

```python
import functools
import math

import jax
import jax.numpy as jnp
from jax import lax
from jax.experimental import pallas as pl
from jax.experimental.pallas import tpu as pltpu
from jax.sharding import Mesh, PartitionSpec as P


COL = ("far", "near")
HD = 128
ROT = 32


NORM_EPS = 1e-05
ROPE_BASE = 10000.0
MASKED = -1e30
SHAMPOO_DECAY = 0.95
MATRIX_RATE = 0.5
WEIGHT_DECAY = 0.01
FIRST_DECAY = 0.9
SECOND_DECAY = 0.95
VECTOR_RATE = 0.6
ADAM_EPS = 1e-08

NT = (((1,), (1,)), ((), ()))
TN = (((0,), (0,)), ((), ()))
NN = (((1,), (0,)), ((), ()))
VMEM_BYTES = 60 * 1024 * 1024


def mm(a, b, dims=NN):
    return lax.dot_general(a, b, dims, preferred_element_type=jnp.float32)


def params(*semantics):
    return pltpu.CompilerParams(dimension_semantics=semantics, vmem_limit_bytes=VMEM_BYTES)


def cost(flops, moved, exps=0):
    return pl.CostEstimate(flops=int(flops), bytes_accessed=int(moved), transcendentals=int(exps))


def whole(shape):
    return pl.BlockSpec(
        shape, lambda *_: (0,) * len(shape), pipeline_mode=pl.Buffered(buffer_count=1)
    )


def halves(tile, width, blocks):
    half = blocks // 2
    return [
        pl.BlockSpec((tile, width), lambda i, _: (jnp.minimum(i, half - 1), 0)),
        pl.BlockSpec((tile, width), lambda i, _: (jnp.maximum(i - half, 0), 0)),
    ]


def assemble(near, width, mine, other, panel_ref):
    half = pl.num_programs(0) // 2
    for number in range(2):

        @pl.when((pl.program_id(0) >= half) == bool(number))
        def _():
            for far in range(panel_ref.shape[1] // (2 * width)):
                at = slice(far * width, (far + 1) * width)
                here = pl.multiple_of((2 * far + near) * width, width)
                there = pl.multiple_of((2 * far + 1 - near) * width, width)
                panel_ref[:, pl.ds(here, width)] = mine[number][:, at]
                panel_ref[:, pl.ds(there, width)] = other[number][:, at]


def positions(lengths, number):
    tokens = jnp.arange(number, dtype=jnp.int32)
    endings = jnp.cumsum(lengths, dtype=jnp.int32)
    finished = (endings[None, :] <= tokens[:, None]).astype(jnp.int32)
    return jnp.sum(finished * lengths[None, :], -1, dtype=jnp.int32)


def rotary_tables(places):
    middle = ROT // 2
    indices = jnp.arange(middle, dtype=jnp.float32)
    inverse = jnp.exp(indices * (-2.0 * math.log(ROPE_BASE) / ROT))
    angles = places.astype(jnp.float32)[:, None] * inverse[None, :]
    cosine, sine = jnp.cos(angles), jnp.sin(angles)
    number = places.shape[0]
    ones = jnp.ones((number, HD - ROT), jnp.float32)
    gap = jnp.zeros((number, middle), jnp.float32)
    rest = jnp.zeros((number, HD - ROT), jnp.float32)
    return (
        jnp.concatenate([cosine, cosine, ones], -1),
        jnp.concatenate([-sine, gap, rest], -1),
        jnp.concatenate([gap, sine, rest], -1),
    )


def turn(vectors, own, ahead, behind):
    middle = ROT // 2
    return (
        vectors * own
        + pltpu.roll(vectors, HD - middle, 1) * ahead
        + pltpu.roll(vectors, middle, 1) * behind
    )


def front_kernel(
    share, near_ref, mine_first, mine_second, other_first, other_second,
    norm_ref, wq_ref, qb_ref, own_ref, ahead_ref, behind_ref, we_ref, eb_ref,
    x_ref, one_ref, two_ref, stat_ref, qkv_ref, act_ref, slope_ref,
):
    assemble(
        near_ref[0], share, (mine_first, mine_second), (other_first, other_second), x_ref
    )
    x = x_ref[...].astype(jnp.float32)
    mu = jnp.mean(x, -1, keepdims=True)
    center = x - mu
    inverse = lax.rsqrt(jnp.mean(center * center, -1, keepdims=True) + NORM_EPS)
    normalized = center * inverse
    stat_ref[...] = jnp.concatenate([mu, inverse], -1)
    one = (normalized * norm_ref[0:1] + norm_ref[1:2]).astype(jnp.bfloat16)
    two = (normalized * norm_ref[2:3] + norm_ref[3:4]).astype(jnp.bfloat16)
    one_ref[...] = one
    two_ref[...] = two
    own, ahead, behind = own_ref[...], ahead_ref[...], behind_ref[...]
    for head in range(wq_ref.shape[1] // (3 * HD)):
        cols = slice(head * 3 * HD, (head + 1) * 3 * HD)
        triple = mm(one, wq_ref[:, cols]) + qb_ref[:, cols]
        query = turn(triple[:, :HD], own, ahead, behind)
        key = turn(triple[:, HD : 2 * HD], own, ahead, behind)
        qkv_ref[:, cols] = jnp.concatenate([query, key, triple[:, 2 * HD :]], -1).astype(
            jnp.bfloat16
        )
    width = 256
    for first in range(0, we_ref.shape[1], width):
        cols = slice(first, first + width)
        hidden = mm(two, we_ref[:, cols]) + eb_ref[:, cols]
        phi = 0.5 + 0.5 * lax.erf(hidden * (0.5**0.5))
        act_ref[:, cols] = (hidden * phi).astype(jnp.bfloat16)
        density = jnp.exp(-0.5 * hidden * hidden) * ((0.5 / math.pi) ** 0.5)
        slope_ref[:, cols] = phi + hidden * density


def front(near, share, mine, other, norm_params, wq, qbias, tables, we, ebias):
    tokens, features = 2 * mine[0].shape[0], 2 * mine[0].shape[1]
    tile = 256
    blocks = tokens // tile
    wide, hidden = wq.shape[1], we.shape[1]

    def rows(width):
        return pl.BlockSpec((tile, width), lambda i, _: (i, 0))

    return pl.pallas_call(
        functools.partial(front_kernel, share),
        grid_spec=pltpu.PrefetchScalarGridSpec(
            num_scalar_prefetch=1,
            grid=(blocks,),
        in_specs=[
            *halves(tile, features // 2, blocks),
            *halves(tile, features // 2, blocks),
            whole(norm_params.shape),
            whole(wq.shape),
            whole((1, wide)),
            rows(HD),
            rows(HD),
            rows(HD),
            whole(we.shape),
            whole((1, hidden)),
        ],
        out_specs=[
            rows(features),
            rows(features),
            rows(features),
            rows(2),
            rows(wide),
            rows(hidden),
            rows(hidden),
        ],
        ),
        out_shape=[
            jax.ShapeDtypeStruct((tokens, features), jnp.bfloat16),
            jax.ShapeDtypeStruct((tokens, features), jnp.bfloat16),
            jax.ShapeDtypeStruct((tokens, features), jnp.bfloat16),
            jax.ShapeDtypeStruct((tokens, 2), jnp.float32),
            jax.ShapeDtypeStruct((tokens, wide), jnp.bfloat16),
            jax.ShapeDtypeStruct((tokens, hidden), jnp.bfloat16),
            jax.ShapeDtypeStruct((tokens, hidden), jnp.float32),
        ],
        compiler_params=params("arbitrary"),
        cost_estimate=cost(
            2 * tokens * features * (wide + hidden), tokens * (6 * features + 2 * wide + 6 * hidden)
        ),
        name="front",
    )(near, *mine, *other, norm_params, wq, qbias[None], *tables, we, ebias[None])


def scores(q, k, rows, begin, start):
    raw = mm(q, k, NT) * HD**-0.5
    cols = start + lax.broadcasted_iota(jnp.int32, raw.shape, 1)
    return raw, (cols >= begin) & (cols <= rows)


def columns(head, kind):
    first = (3 * head + kind) * HD
    return slice(first, first + HD)


def attend_kernel(from_ref, qkv_ref, begin_ref, out_ref, sum_ref, held):
    tile, span = begin_ref.shape[0], held.shape[3]
    heads = range(held.shape[0])
    block = pl.program_id(0)
    low, high = from_ref[block], (block * tile + tile - 1) // span + 1
    begin = begin_ref[...]
    here = pl.ds(pl.multiple_of(block * tile, tile), tile)
    queries = [qkv_ref[here, columns(h, 0)] for h in heads]
    rows = block * tile + lax.broadcasted_iota(jnp.int32, (tile, 1), 0)

    def first_pass(j, tops):
        start = pl.multiple_of(j * span, span)
        part = pl.ds(start, span)
        out = []
        for h in heads:
            raw, allowed = scores(queries[h], qkv_ref[part, columns(h, 1)], rows, begin, start)
            raw = jnp.where(allowed, raw, MASKED)
            held[h, j] = raw
            out.append(jnp.maximum(tops[h], jnp.max(raw, -1, keepdims=True)))
        return tuple(out)

    least = jnp.full((tile, 1), MASKED, jnp.float32)
    tops = lax.fori_loop(low, high, first_pass, tuple(least for _ in heads))

    def second_pass(j, carry):
        part = pl.ds(pl.multiple_of(j * span, span), span)
        out = []
        for h in heads:
            weights = jnp.exp(held[h, j] - tops[h])
            total = carry[h][0] + jnp.sum(weights, -1, keepdims=True)
            mixed = mm(weights.astype(jnp.bfloat16), qkv_ref[part, columns(h, 2)])
            out.append((total, carry[h][1] + mixed))
        return tuple(out)

    empty = (jnp.zeros((tile, 1), jnp.float32), jnp.zeros((tile, HD), jnp.float32))
    done = lax.fori_loop(low, high, second_pass, tuple(empty for _ in heads))
    for h in heads:
        total, out = done[h]
        out_ref[:, h * HD : (h + 1) * HD] = (out / total).astype(jnp.bfloat16)
        sum_ref[h] = tops[h] + jnp.log(total)


def tiles(length):
    return min(256, length), min(512, length)


def attend(qkv, begin):
    length = qkv.shape[0]
    heads = qkv.shape[1] // (3 * HD)
    tile, span = tiles(length)
    grid_spec = pltpu.PrefetchScalarGridSpec(
        num_scalar_prefetch=1,
        grid=(length // tile,),
        in_specs=[whole(qkv.shape), pl.BlockSpec((tile, 1), lambda i, _: (i, 0))],
        out_specs=[
            pl.BlockSpec((tile, heads * HD), lambda i, _: (i, 0)),
            pl.BlockSpec((heads, tile, 1), lambda i, _: (0, i, 0)),
        ],
        scratch_shapes=[pltpu.VMEM((heads, length // span, tile, span), jnp.float32)],
    )
    return pl.pallas_call(
        attend_kernel,
        grid_spec=grid_spec,
        out_shape=[
            jax.ShapeDtypeStruct((length, heads * HD), jnp.bfloat16),
            jax.ShapeDtypeStruct((heads, length, 1), jnp.float32),
        ],
        compiler_params=params("arbitrary"),
        cost_estimate=cost(4 * heads * length * length * HD, 8 * heads * length * HD, heads * length * length),
        name="attend",
    )(begin[::tile] // span, qkv, begin[:, None])


def attend_back_kernel(
    from_ref, qkv_ref, grad_ref, begin_ref, sum_ref, own_ref, ahead_ref, behind_ref,
    out_ref, probs, probs_back, key_back, value_back,
):
    tile, span = begin_ref.shape[0], probs.shape[3]
    heads = range(probs.shape[0])
    block, blocks = pl.program_id(0), pl.num_programs(0)
    low, high = from_ref[block], (block * tile + tile - 1) // span + 1
    begin = begin_ref[...]
    here = pl.ds(pl.multiple_of(block * tile, tile), tile)
    queries = [qkv_ref[here, columns(h, 0)] for h in heads]
    grads = [grad_ref[:, h * HD : (h + 1) * HD] for h in heads]
    rows = block * tile + lax.broadcasted_iota(jnp.int32, (tile, 1), 0)

    @pl.when(block == 0)
    def _():
        key_back[...] = jnp.zeros_like(key_back)
        value_back[...] = jnp.zeros_like(value_back)

    def first_pass(j, inner):
        start = pl.multiple_of(j * span, span)
        part = pl.ds(start, span)
        out = []
        for h in heads:
            raw, allowed = scores(queries[h], qkv_ref[part, columns(h, 1)], rows, begin, start)
            weights = jnp.where(allowed, jnp.exp(raw - sum_ref[h]), 0.0)
            back = mm(grads[h], qkv_ref[part, columns(h, 2)], NT)
            probs[h, j] = weights
            probs_back[h, j] = back
            out.append(inner[h] + jnp.sum(weights * back, -1, keepdims=True))
        return tuple(out)

    zero = jnp.zeros((tile, 1), jnp.float32)
    inner = lax.fori_loop(low, high, first_pass, tuple(zero for _ in heads))

    def second_pass(j, query_back):
        part = pl.ds(pl.multiple_of(j * span, span), span)
        out = []
        for h in heads:
            weights = probs[h, j]
            raw_back = (weights * (probs_back[h, j] - inner[h]) * HD**-0.5).astype(jnp.bfloat16)
            key_back[h, part] += mm(raw_back, queries[h], TN)
            value_back[h, part] += mm(weights.astype(jnp.bfloat16), grads[h], TN)
            out.append(query_back[h] + mm(raw_back, qkv_ref[part, columns(h, 1)]))
        return tuple(out)

    empty = jnp.zeros((tile, HD), jnp.float32)
    query_back = lax.fori_loop(low, high, second_pass, tuple(empty for _ in heads))
    for h in heads:
        turned = turn(query_back[h], own_ref[here], -ahead_ref[here], -behind_ref[here])
        out_ref[here, columns(h, 0)] = turned.astype(jnp.bfloat16)

    @pl.when(block == blocks - 1)
    def _():
        def finish(i, _):
            at = pl.ds(pl.multiple_of(i * tile, tile), tile)
            for h in heads:
                keys = turn(key_back[h, at], own_ref[at], -ahead_ref[at], -behind_ref[at])
                out_ref[at, columns(h, 1)] = keys.astype(jnp.bfloat16)
                out_ref[at, columns(h, 2)] = value_back[h, at].astype(jnp.bfloat16)
            return 0

        lax.fori_loop(0, blocks, finish, 0)


def attend_back(qkv, begin, grad, logsum, tables):
    length = qkv.shape[0]
    heads = qkv.shape[1] // (3 * HD)
    tile, span = tiles(length)
    grid_spec = pltpu.PrefetchScalarGridSpec(
        num_scalar_prefetch=1,
        grid=(length // tile,),
        in_specs=[
            whole(qkv.shape),
            pl.BlockSpec((tile, heads * HD), lambda i, _: (i, 0)),
            pl.BlockSpec((tile, 1), lambda i, _: (i, 0)),
            pl.BlockSpec((heads, tile, 1), lambda i, _: (0, i, 0)),
            whole((length, HD)),
            whole((length, HD)),
            whole((length, HD)),
        ],
        out_specs=[pl.BlockSpec(qkv.shape, lambda i, _: (0, 0))],
        scratch_shapes=[
            pltpu.VMEM((heads, length // span, tile, span), jnp.float32),
            pltpu.VMEM((heads, length // span, tile, span), jnp.float32),
            pltpu.VMEM((heads, length, HD), jnp.float32),
            pltpu.VMEM((heads, length, HD), jnp.float32),
        ],
    )
    return pl.pallas_call(
        attend_back_kernel,
        grid_spec=grid_spec,
        out_shape=[jax.ShapeDtypeStruct(qkv.shape, jnp.bfloat16)],
        compiler_params=params("arbitrary"),
        cost_estimate=cost(10 * heads * length * length * HD, 14 * heads * length * HD, heads * length * length),
        name="attend_back",
    )(begin[::tile] // span, qkv, grad, begin[:, None], logsum, *tables)[0]


def join_kernel(
    share, near_ref, a_ref, wa_ref, b_ref, wb_ref,
    keep_first, keep_second, away_first, away_second,
):
    near = near_ref[0]
    a, b = a_ref[...], b_ref[...]
    half = pl.num_programs(0) // 2
    for number, keep_ref, away_ref in (
        (0, keep_first, away_first),
        (1, keep_second, away_second),
    ):

        @pl.when((pl.program_id(0) >= half) == bool(number))
        def _():
            def far(f, _):
                at = pl.ds(pl.multiple_of(f * share, share), share)
                here = pl.ds(pl.multiple_of((2 * f + near) * share, share), share)
                there = pl.ds(pl.multiple_of((2 * f + 1 - near) * share, share), share)
                keep_ref[:, at] = mm(a, wa_ref[:, here]) + mm(b, wb_ref[:, here])
                away = mm(a, wa_ref[:, there]) + mm(b, wb_ref[:, there])
                away_ref[:, at] = away.astype(jnp.bfloat16)
                return 0

            lax.fori_loop(0, keep_ref.shape[1] // share, far, 0, unroll=True)


def join(near, share, a, wa, b, wb):
    tokens, features = a.shape[0], wa.shape[1]
    tile = 256
    blocks = tokens // tile
    half = (tokens // 2, features // 2)
    return pl.pallas_call(
        functools.partial(join_kernel, share),
        grid_spec=pltpu.PrefetchScalarGridSpec(
            num_scalar_prefetch=1,
            grid=(blocks,),
            in_specs=[
                pl.BlockSpec((tile, a.shape[1]), lambda i, _: (i, 0)),
                whole(wa.shape),
                pl.BlockSpec((tile, b.shape[1]), lambda i, _: (i, 0)),
                whole(wb.shape),
            ],
            out_specs=[
                *halves(tile, features // 2, blocks),
                *halves(tile, features // 2, blocks),
            ],
        ),
        out_shape=[
            jax.ShapeDtypeStruct(half, jnp.float32),
            jax.ShapeDtypeStruct(half, jnp.float32),
            jax.ShapeDtypeStruct(half, jnp.bfloat16),
            jax.ShapeDtypeStruct(half, jnp.bfloat16),
        ],
        compiler_params=params("arbitrary"),
        cost_estimate=cost(2 * tokens * features * (a.shape[1] + b.shape[1]), 6 * tokens * features),
        name="join",
    )(near, a, wa, b, wb)


def part_kernel(
    share, near_ref, mine_first, mine_second, other_first, other_second,
    wd_ref, wr_ref, slope_ref, g_ref, att_ref, hid_ref, sum_ref,
):
    assemble(
        near_ref[0], share, (mine_first, mine_second), (other_first, other_second), g_ref
    )
    g = g_ref[...]
    att_ref[...] = mm(g, wd_ref[...], NT).astype(jnp.bfloat16)

    @pl.when(pl.program_id(0) == 0)
    def _():
        sum_ref[...] = jnp.zeros_like(sum_ref)

    width = 256
    for first in range(0, wr_ref.shape[0], width):
        cols = slice(first, first + width)
        back = (mm(g, wr_ref[cols], NT) * slope_ref[:, cols]).astype(jnp.bfloat16)
        hid_ref[:, cols] = back
        sum_ref[:, cols] += jnp.sum(back.astype(jnp.float32), 0, keepdims=True)


def part(near, share, mine, other, wd, wr, slope):
    tokens, features = 2 * mine[0].shape[0], 2 * mine[0].shape[1]
    tile = 256
    blocks = tokens // tile

    def rows(width):
        return pl.BlockSpec((tile, width), lambda i, _: (i, 0))

    return pl.pallas_call(
        functools.partial(part_kernel, share),
        grid_spec=pltpu.PrefetchScalarGridSpec(
            num_scalar_prefetch=1,
            grid=(blocks,),
        in_specs=[
            *halves(tile, features // 2, blocks),
            *halves(tile, features // 2, blocks),
            whole(wd.shape),
            whole(wr.shape),
            rows(wr.shape[0]),
        ],
        out_specs=[
            rows(features),
            rows(wd.shape[0]),
            rows(wr.shape[0]),
            pl.BlockSpec((1, wr.shape[0]), lambda i, _: (0, 0)),
        ],
        ),
        out_shape=[
            jax.ShapeDtypeStruct((tokens, features), jnp.bfloat16),
            jax.ShapeDtypeStruct((tokens, wd.shape[0]), jnp.bfloat16),
            jax.ShapeDtypeStruct((tokens, wr.shape[0]), jnp.bfloat16),
            jax.ShapeDtypeStruct((1, wr.shape[0]), jnp.float32),
        ],
        compiler_params=params("arbitrary"),
        cost_estimate=cost(
            2 * tokens * features * (wd.shape[0] + wr.shape[0]), tokens * (2 * features + 8 * wr.shape[0])
        ),
        name="part",
    )(near, *mine, *other, wd, wr, slope)


def back_kernel(
    share, near_ref, tb_ref, wq_ref, hb_ref, we_ref, x_ref, stat_ref, norm_ref,
    keep_first, keep_second, away_first, away_second, row_ref, col_ref,
):
    near = near_ref[0]
    half = pl.num_programs(0) // 2

    @pl.when(pl.program_id(0) == 0)
    def _():
        col_ref[...] = jnp.zeros_like(col_ref)

    triple_back, hidden_back = tb_ref[...], hb_ref[...]
    mu, inverse = stat_ref[:, 0:1], stat_ref[:, 1:2]

    def block(number, plain, crossed):
        cols = pl.ds(pl.multiple_of(number * share, share), share)
        one = mm(triple_back, wq_ref[cols], NT)
        two = mm(hidden_back, we_ref[cols], NT)
        normalized = (x_ref[:, cols].astype(jnp.float32) - mu) * inverse
        col_ref[:, cols] += jnp.concatenate(
            [
                jnp.sum(one * normalized, 0, keepdims=True),
                jnp.sum(one, 0, keepdims=True),
                jnp.sum(two * normalized, 0, keepdims=True),
                jnp.sum(two, 0, keepdims=True),
            ],
            0,
        )
        both = one * norm_ref[0:1, cols] + two * norm_ref[2:3, cols]
        plain = plain + jnp.sum(both, -1, keepdims=True)
        return both, plain, crossed + jnp.sum(both * normalized, -1, keepdims=True)

    zero = jnp.zeros((tb_ref.shape[0], 1), jnp.float32)
    for number, keep_ref, away_ref in (
        (0, keep_first, away_first),
        (1, keep_second, away_second),
    ):

        @pl.when((pl.program_id(0) >= half) == bool(number))
        def _():
            def far(f, carry):
                at = pl.ds(pl.multiple_of(f * share, share), share)
                both, plain, crossed = block(2 * f + near, *carry)
                keep_ref[:, at] = both
                both, plain, crossed = block(2 * f + 1 - near, plain, crossed)
                away_ref[:, at] = both.astype(jnp.bfloat16)
                return plain, crossed

            plain, crossed = lax.fori_loop(
                0, keep_ref.shape[1] // share, far, (zero, zero), unroll=True
            )
            row_ref[...] = jnp.concatenate([plain, crossed], -1)


def back(near, share, triple_back, wq, hidden_back, we, panel, stats, norm_params):
    tokens, features = panel.shape
    tile = 256
    blocks = tokens // tile
    half = (tokens // 2, features // 2)

    def rows(width):
        return pl.BlockSpec((tile, width), lambda i, _: (i, 0))

    return pl.pallas_call(
        functools.partial(back_kernel, share),
        grid_spec=pltpu.PrefetchScalarGridSpec(
            num_scalar_prefetch=1,
            grid=(blocks,),
            in_specs=[
                rows(wq.shape[1]),
                whole(wq.shape),
                rows(we.shape[1]),
                whole(we.shape),
                rows(features),
                rows(2),
                whole(norm_params.shape),
            ],
            out_specs=[
                *halves(tile, features // 2, blocks),
                *halves(tile, features // 2, blocks),
                rows(2),
                pl.BlockSpec((4, features), lambda i, _: (0, 0)),
            ],
        ),
        out_shape=[
            jax.ShapeDtypeStruct(half, jnp.float32),
            jax.ShapeDtypeStruct(half, jnp.float32),
            jax.ShapeDtypeStruct(half, jnp.bfloat16),
            jax.ShapeDtypeStruct(half, jnp.bfloat16),
            jax.ShapeDtypeStruct((tokens, 2), jnp.float32),
            jax.ShapeDtypeStruct((4, features), jnp.float32),
        ],
        compiler_params=params("arbitrary"),
        cost_estimate=cost(
            2 * tokens * features * (wq.shape[1] + we.shape[1]), tokens * 8 * features
        ),
        name="back",
    )(near, triple_back, wq, hidden_back, we, panel, stats, norm_params)


def shampoo_kernel(scaling, w_ref, g_ref, l_ref, r_ref, p_ref, q_ref, nw_ref, nl_ref, nr_ref):
    size = l_ref.shape[-1]
    for block in range(l_ref.shape[1]):
        cols = slice(block * size, (block + 1) * size)
        grad = (g_ref[:, cols] * scaling).astype(jnp.bfloat16)
        nl_ref[0, block] = SHAMPOO_DECAY * l_ref[0, block] + (1.0 - SHAMPOO_DECAY) * mm(grad, grad, NT)
        nr_ref[0, block] = SHAMPOO_DECAY * r_ref[0, block] + (1.0 - SHAMPOO_DECAY) * mm(grad, grad, TN)
        turned = mm(p_ref[0, block].astype(jnp.bfloat16), grad).astype(jnp.bfloat16)
        step = mm(turned, q_ref[0, block].astype(jnp.bfloat16))
        weight = w_ref[:, cols]
        nw_ref[:, cols] = weight - MATRIX_RATE * (step + WEIGHT_DECAY * weight)


def shampoo(weight, gradient, left_stat, right_stat, left_root, right_root, scaling):
    height, breadth = gradient.shape
    size = left_stat.shape[-1]
    across = breadth // size
    flat = pl.BlockSpec((size, breadth), lambda i: (i, 0))
    cube = pl.BlockSpec((1, across, size, size), lambda i: (i, 0, 0, 0))
    return pl.pallas_call(
        functools.partial(shampoo_kernel, scaling),
        grid=(height // size,),
        in_specs=[flat, flat, cube, cube, cube, cube],
        out_specs=[flat, cube, cube],
        out_shape=[
            jax.ShapeDtypeStruct(weight.shape, jnp.float32),
            jax.ShapeDtypeStruct(left_stat.shape, jnp.float32),
            jax.ShapeDtypeStruct(right_stat.shape, jnp.float32),
        ],
        compiler_params=params("arbitrary"),
        cost_estimate=cost(8 * height * breadth * size, 36 * height * breadth),
    )(weight, gradient, left_stat, right_stat, left_root, right_root)


def swap(value, axis, bit):
    size = lax.axis_size(axis)
    return lax.ppermute(value, axis, [(i, i ^ bit) for i in range(size)])


def gather_row(shard, dim):
    if lax.axis_size("row") != 4:
        return lax.all_gather(shard, "row", axis=dim, tiled=True)
    me = lax.axis_index("row")
    across = swap(shard, "row", 2)
    beside = swap(shard, "row", 1)
    corner = swap(across, "row", 1)
    shape = list(shard.shape)
    step = shape[dim]
    shape[dim] *= 4
    out = jnp.zeros(shape, shard.dtype)
    for bit, piece in ((0, shard), (2, across), (1, beside), (3, corner)):
        out = lax.dynamic_update_slice_in_dim(out, piece, (me ^ bit) * step, dim)
    return out


def scatter_row(value, dim):
    if lax.axis_size("row") != 4:
        return lax.psum_scatter(value, "row", scatter_dimension=dim, tiled=True)
    me = lax.axis_index("row")
    step = value.shape[dim] // 4

    def share(owner):
        return lax.dynamic_slice_in_dim(value, owner * step, step, dim)

    far_beside = swap(share(me ^ 3).astype(jnp.bfloat16), "row", 1)
    near_beside = swap(share(me ^ 1).astype(jnp.bfloat16), "row", 1)
    far = share(me ^ 2) + far_beside.astype(jnp.float32)
    across = swap(far.astype(jnp.bfloat16), "row", 2)
    return share(me) + near_beside.astype(jnp.float32) + across.astype(jnp.float32)


def total(value, axes):
    for axis in axes:
        bit = 1
        while bit < lax.axis_size(axis):
            value = value + swap(value, axis, bit)
            bit *= 2
    return value


def gather_far(value):
    half = value.shape[0] // 2
    return [
        lax.all_gather(value[first : first + half], "far", axis=1, tiled=True)
        for first in (0, half)
    ]


def scatter_far(both):
    return lax.psum_scatter(both, "far", scatter_dimension=1, tiled=True)


def pair_sum(kept, received):
    return (kept + received.astype(jnp.float32)).astype(jnp.bfloat16)


def product(a, b):
    return mm(a, b, TN)


def after(value, *others):
    return lax.optimization_barrier((value, *others))[0]


def adam(vector, moment_one, moment_two, gradient, scaling, counter):
    mean_grad = gradient * scaling
    new_one = FIRST_DECAY * moment_one + (1.0 - FIRST_DECAY) * mean_grad
    new_two = SECOND_DECAY * moment_two + (1.0 - SECOND_DECAY) * mean_grad * mean_grad
    first_hat = new_one / (1.0 - FIRST_DECAY**counter)
    second_hat = new_two / (1.0 - SECOND_DECAY**counter)
    new_vector = vector - VECTOR_RATE * first_hat / (jnp.sqrt(second_hat) + ADAM_EPS)
    return (new_vector, new_one, new_two)


def local(
    tokens_in,
    grad_out,
    sequence_lengths,
    step_count,
    query_key_value,
    attn_dense,
    mlp_expand,
    mlp_reduce,
    norm_params,
    query_bias,
    dense_biases,
    expand_bias,
    norm_first,
    norm_second,
    query_bias_first,
    query_bias_second,
    dense_biases_first,
    dense_biases_second,
    expand_bias_first,
    expand_bias_second,
    query_left,
    query_right,
    attn_left,
    attn_right,
    expand_left,
    expand_right,
    reduce_left,
    reduce_right,
    query_left_root,
    query_right_root,
    attn_left_root,
    attn_right_root,
    expand_left_root,
    expand_right_root,
    reduce_left_root,
    reduce_right_root,
):
    input_mine, cotangent_mine = gather_far(tokens_in), gather_far(grad_out)
    input_other = [swap(piece, "near", 1) for piece in input_mine]
    query_full = gather_row(query_key_value.astype(jnp.bfloat16), 0)
    expand_full = gather_row(mlp_expand.astype(jnp.bfloat16), 0)
    dense_full = gather_row(attn_dense.astype(jnp.bfloat16), 1)
    reduce_full = gather_row(mlp_reduce.astype(jnp.bfloat16), 1)
    row_count, col_width = tokens_in.shape
    features = norm_params.shape[1]
    near = lax.axis_index("near").astype(jnp.int32)[None]
    begin = positions(sequence_lengths[0], row_count)
    tables = rotary_tables(jnp.arange(row_count, dtype=jnp.int32) - begin)
    input_panel, first_in, second_in, stats, qkv, activated, slope = front(
        after(near, dense_full, reduce_full), col_width, input_mine, input_other, norm_params,
        query_full, query_bias, tables, expand_full, expand_bias,
    )
    cotangent_other = [
        swap(cotangent_mine[0], "near", 1), swap(after(cotangent_mine[1], stats), "near", 1)
    ]
    attended, logsum = attend(qkv, begin)
    *branches_kept, sent_first, sent_second = join(
        near, col_width, attended, dense_full, activated, reduce_full
    )
    branches_got = [swap(sent_first, "near", 1), swap(sent_second, "near", 1)]
    output_sum = jnp.sum(after(grad_out, sent_first), 0, dtype=jnp.float32)
    cotangent_panel, attended_back, hidden_back, hidden_sum = part(
        near, col_width, cotangent_mine, cotangent_other, dense_full, reduce_full,
        after(slope, sent_first),
    )
    triple_back = attend_back(qkv, begin, attended_back, logsum, tables)
    branch_sum = pair_sum(branches_kept[0], after(branches_got[0], triple_back))
    branch_first = scatter_far(branch_sum)
    *both_kept, sent_first, sent_second, row_sums, norm_grad = back(
        near, col_width, after(triple_back, branch_sum), query_full, hidden_back, expand_full,
        input_panel, stats, norm_params,
    )
    both_got = [swap(sent_first, "near", 1), swap(sent_second, "near", 1)]
    cotangent_late = after(cotangent_panel, sent_first)
    reduce_part = product(activated, cotangent_late)
    reduce_grad = scatter_row(reduce_part, 1)
    dense_part = product(attended, cotangent_late)
    dense_grad = scatter_row(dense_part, 1)
    branch_sum = pair_sum(branches_kept[1], after(branches_got[1], dense_part, reduce_part))
    branch_second = scatter_far(branch_sum)
    expand_part = product(after(second_in, branch_sum), hidden_back)
    expand_grad = scatter_row(expand_part, 0)
    first_sum = pair_sum(both_kept[0], after(both_got[0], expand_part))
    both_first = scatter_far(first_sum)
    qkv_part = product(after(first_in, first_sum), triple_back)
    qkv_grad = scatter_row(qkv_part, 0)
    lanes = 128
    row_sums = total(row_sums.T.reshape(-1, lanes), ("near", "far")).reshape(2, row_count)
    norm_total = total(norm_grad.reshape(-1, lanes), ("near", "far", "row")).reshape(4, features)
    sums = jnp.concatenate(
        [jnp.sum(triple_back, 0, dtype=jnp.float32), output_sum, hidden_sum[0]]
    )
    sums = total(sums.reshape(-1, lanes), ("row",)).reshape(-1)
    query_bias_total = sums[: query_bias.shape[0]]
    output_total = sums[query_bias.shape[0] : query_bias.shape[0] + col_width]
    dense_total = jnp.stack([output_total, output_total])
    expand_total = sums[query_bias.shape[0] + col_width :]
    norm_slice = (tokens_in.astype(jnp.float32) - stats[:, 0:1]) * stats[:, 1:2]
    scaling = 1.0 / (row_count * lax.axis_size("row"))
    counter = step_count[0].astype(jnp.float32)
    new_dense, new_attn_left, new_attn_right = shampoo(
        attn_dense,
        after(dense_grad, qkv_part, expand_part),
        attn_left,
        attn_right,
        attn_left_root,
        attn_right_root,
        scaling,
    )
    new_reduce, new_reduce_left, new_reduce_right = shampoo(
        mlp_reduce,
        after(reduce_grad, qkv_part, expand_part),
        reduce_left,
        reduce_right,
        reduce_left_root,
        reduce_right_root,
        scaling,
    )
    second_sum = pair_sum(both_kept[1], after(both_got[1], new_dense, new_reduce))
    both_second = scatter_far(second_sum)
    new_qkv, new_query_left, new_query_right = shampoo(
        query_key_value,
        after(qkv_grad, second_sum),
        query_left,
        query_right,
        query_left_root,
        query_right_root,
        scaling,
    )
    new_expand, new_expand_left, new_expand_right = shampoo(
        mlp_expand,
        after(expand_grad, second_sum),
        expand_left,
        expand_right,
        expand_left_root,
        expand_right_root,
        scaling,
    )
    branch_share = jnp.concatenate([branch_first, after(branch_second, new_qkv)], 0)
    branch_share = branch_share.astype(jnp.float32)
    both = jnp.concatenate([both_first, after(both_second, new_qkv, new_expand)], 0)
    both = both.astype(jnp.float32)
    block_out = tokens_in.astype(jnp.float32) + branch_share + dense_biases[0] + dense_biases[1]
    mean = (row_sums[0] / features)[:, None]
    cross = (row_sums[1] / features)[:, None]
    tokens_grad = grad_out.astype(jnp.float32) + stats[:, 1:2] * (
        both - mean - norm_slice * cross
    )
    new_norm, new_norm_one, new_norm_two = adam(
        norm_params, norm_first, norm_second, norm_total, scaling, counter
    )
    new_qbias, new_qbias_one, new_qbias_two = adam(
        query_bias, query_bias_first, query_bias_second, query_bias_total, scaling, counter
    )
    new_dbias, new_dbias_one, new_dbias_two = adam(
        dense_biases, dense_biases_first, dense_biases_second, dense_total, scaling, counter
    )
    new_ebias, new_ebias_one, new_ebias_two = adam(
        expand_bias, expand_bias_first, expand_bias_second, expand_total, scaling, counter
    )
    return (
        block_out,
        tokens_grad,
        qkv_grad,
        dense_grad,
        expand_grad,
        reduce_grad,
        new_qkv,
        new_dense,
        new_expand,
        new_reduce,
        new_query_left,
        new_query_right,
        new_attn_left,
        new_attn_right,
        new_expand_left,
        new_expand_right,
        new_reduce_left,
        new_reduce_right,
        new_norm,
        new_norm_one,
        new_norm_two,
        new_qbias,
        new_qbias_one,
        new_qbias_two,
        new_dbias,
        new_dbias_one,
        new_dbias_two,
        new_ebias,
        new_ebias_one,
        new_ebias_two,
    )


def solution(mesh):
    rows, cols = mesh.shape["row"], mesh.shape["col"]
    split = Mesh(mesh.devices.reshape(rows, cols // 2, 2), ("row", *COL))
    return jax.shard_map(
        local,
        mesh=split,
        in_specs=(
            P("row", COL),
            P("row", COL),
            P("row", None),
            P(),
            P("row", COL),
            P(COL, "row"),
            P("row", COL),
            P(COL, "row"),
            P(),
            P(COL),
            P(None, COL),
            P(COL),
            P(),
            P(),
            P(COL),
            P(COL),
            P(None, COL),
            P(None, COL),
            P(COL),
            P(COL),
            P("row", COL, None, None),
            P("row", COL, None, None),
            P(COL, "row", None, None),
            P(COL, "row", None, None),
            P("row", COL, None, None),
            P("row", COL, None, None),
            P(COL, "row", None, None),
            P(COL, "row", None, None),
            P("row", COL, None, None),
            P("row", COL, None, None),
            P(COL, "row", None, None),
            P(COL, "row", None, None),
            P("row", COL, None, None),
            P("row", COL, None, None),
            P(COL, "row", None, None),
            P(COL, "row", None, None),
        ),
        out_specs=(
            P("row", COL),
            P("row", COL),
            P("row", COL),
            P(COL, "row"),
            P("row", COL),
            P(COL, "row"),
            P("row", COL),
            P(COL, "row"),
            P("row", COL),
            P(COL, "row"),
            P("row", COL, None, None),
            P("row", COL, None, None),
            P(COL, "row", None, None),
            P(COL, "row", None, None),
            P("row", COL, None, None),
            P("row", COL, None, None),
            P(COL, "row", None, None),
            P(COL, "row", None, None),
            P(),
            P(),
            P(),
            P(COL),
            P(COL),
            P(COL),
            P(None, COL),
            P(None, COL),
            P(None, COL),
            P(COL),
            P(COL),
            P(COL),
        ),
        check_vma=False,
    )
```
